512 devices in a mesh: seq: 128 (over y, z, core), head: 4 (over x).
Axes of the slice: x: 4, y: 8, z: 8, core: 2. Of those that a mesh axis runs over, the one named last changes fastest.
Arguments:
- hidden_states: bfloat16 [8, 8192, 3584], P(None, 'seq', 'head'), may hold values from -6 to 6
- boundary: int32 [8, 64], replicated, may hold values from 0 to 8191, as said below
- valid: int32 [8, 64], replicated, may hold values from 0 to 1, as said below
- pairs: int32 [8, 2], replicated, may hold values from 0 to 7, as said below
- w_first: bfloat16 [3584, 4096], P('seq', 'head'), may hold values from -0.09375 to 0.09375
- b_first: float32 [4096], P('head'), may hold values from -3 to 3
- w_second: float32 [4096], P('head'), may hold values from -0.09375 to 0.09375
Outputs:
- step_reward: float32 [8, 64], replicated
- trace_score: float32 [8], replicated
- margin: float32 [8], replicated
The draws below stay inside these ranges and needn't reach their ends.
Inputs may be any that keep to these rules, and one draw needn't show every extreme that they name: Within a trace the 64 boundary positions are distinct and increasing. In each trace the ones come first; every trace has 16 to 64 valid steps. `pairs`: the two traces of a pair differ.
All inputs are finite; a program needn't handle non-finite values.
Results may differ from the reference program's by a relative error of at most 0.0003.
Values may be sent and summed in bfloat16 or wider, within the bound.
No kernel may reach another device: no remote copies, remote signals or barrier semaphores. Data moves between devices by JAX's collectives and lax.ppermute only.
A program may use at most 64 MiB of HBM per device.

```python
import jax
import jax.numpy as jnp

D = 3584
HID = 4096
STEPS = 64
TRACES = 8
SEQLEN = 8192
PAIRS = 8


def count_steps(key):
    return jax.random.randint(jax.random.fold_in(key, 11), (TRACES,), 16, STEPS + 1)


def draw_boundary(key, part):
    keys = jax.random.split(jax.random.fold_in(key, 23), TRACES)

    def one_trace(single):
        chosen = jax.random.permutation(single, SEQLEN)[:STEPS]
        return jnp.sort(chosen)
    return jax.vmap(one_trace)(keys).astype(jnp.int32)


def draw_valid(key, part):
    counts = count_steps(key)
    slots = jnp.arange(STEPS)[None, :]
    return (slots < counts[:, None]).astype(jnp.int32)


def draw_pairs(key, part):
    first = jax.random.randint(jax.random.fold_in(key, 31), (PAIRS,), 0, TRACES)
    offset = jax.random.randint(jax.random.fold_in(key, 37), (PAIRS,), 1, TRACES)
    second = (first + offset) % TRACES
    return jnp.stack([first, second], axis=1).astype(jnp.int32)


def block_scale(rng, dims, shards, smallest, top_value):
    def one(position, parts):
        draws = jax.random.uniform(jax.random.fold_in(jax.random.fold_in(rng, 6), position), (parts,), jnp.float32, smallest / len(shards), top_value / len(shards))
        return jnp.repeat(jnp.exp(draws), dims[position] // parts).reshape((-1,) + (1,) * (len(dims) - position - 1))

    level = one(*shards[0])
    for cut in shards[1:]:
        level = level * one(*cut)
    return level


def noise(key, extent, spread, most, pieces=(), kind=jnp.bfloat16):
    loudness = block_scale(key, extent, pieces, -0.22, 0.18) if pieces else 1.0
    entries = jax.random.normal(key, extent, jnp.float32) * spread * loudness
    return jnp.minimum(jnp.maximum(entries, -most), most).astype(kind)


def setup_inputs(seed: int = 0) -> dict:
    arg_keys = jax.random.split(jax.random.key(seed), 8)
    hidden_states = noise(arg_keys[0], (TRACES, SEQLEN, D), 1.0, 6.0, ((1, 128), (2, 4)))
    boundary = draw_boundary(jax.random.fold_in(arg_keys[7], 71), 0)
    valid = draw_valid(jax.random.fold_in(arg_keys[7], 71), 0)
    pairs = draw_pairs(jax.random.fold_in(arg_keys[7], 71), 0)
    w_first = noise(arg_keys[4], (D, HID), D ** -0.5, 0.09375, ((0, 128), (1, 4)))
    b_first = noise(arg_keys[5], (HID,), 0.5, 3.0, ((0, 4),), jnp.float32)
    w_second = noise(arg_keys[6], (HID,), HID ** -0.5, 0.09375, ((0, 4),), jnp.float32)
    return dict(hidden_states=hidden_states, boundary=boundary, valid=valid, pairs=pairs, w_first=w_first, b_first=b_first, w_second=w_second)


def reference(hidden_states, boundary, valid, pairs, w_first, b_first, w_second):
    picked = jnp.take_along_axis(hidden_states, boundary[:, :, None].astype(jnp.int32), axis=1)
    rows = picked.reshape(TRACES * STEPS, D)
    pre = jnp.dot(rows, w_first, preferred_element_type=jnp.float32) + b_first
    logit = jnp.sum(jnp.maximum(pre, 0.0) * w_second, axis=-1).reshape(TRACES, STEPS)
    live = valid == 1
    step_reward = jnp.where(live, logit, jnp.float32(0.0))
    trace_score = jnp.min(jnp.where(live, logit, jnp.float32(1e30)), axis=1)
    margin = trace_score[pairs[:, 0]] - trace_score[pairs[:, 1]]
    return step_reward, trace_score, margin
```

```python
import jax
import jax.numpy as jnp
from jax import lax
from jax.experimental import pallas as pl
from jax.experimental.pallas import tpu as pltpu
from jax.sharding import Mesh
from jax.sharding import PartitionSpec as P

NY, NZ, NC, NX = 8, 8, 2, 4
ZC = NZ * NC
SEQ = ("y", "z", "c")
XZC = ("x", "z", "c")
ALL = ("y", "z", "c", "x")
SLOTS = 16
ROUND_SLOTS = 6
CAP = 96
HALF = CAP // 2
VMEM = pl.BlockSpec(memory_space=pltpu.VMEM)
SMEM = pl.BlockSpec(memory_space=pltpu.SMEM)
F32, BF16, I32 = jnp.float32, jnp.bfloat16, jnp.int32
HIGH = lax.Precision.HIGHEST


def iota(shape, dim):
    return lax.broadcasted_iota(I32, shape, dim)


def pick_kernel(scalars, boundary_ref, hidden_ref, out_ref):
    me, low = scalars[0], scalars[1]
    traces, steps = boundary_ref.shape
    tokens = hidden_ref.shape[1]
    bound = boundary_ref[...]
    local = bound - me * tokens
    mine = (local >= 0) & (local < tokens)
    owned = jnp.where(mine, 1.0, 0.0).astype(BF16)
    before = jnp.where(iota((steps, steps), 0) < iota((steps, steps), 1), 1.0, 0.0).astype(BF16)
    within = jnp.dot(owned, before, preferred_element_type=F32)
    totals = jnp.dot(owned, jnp.ones((steps, steps), BF16), preferred_element_type=F32)
    earlier = jnp.where(iota((traces, traces), 1) < iota((traces, traces), 0), 1.0, 0.0)
    carried = jnp.dot(earlier.astype(BF16), totals.astype(BF16), preferred_element_type=F32)
    slot = jnp.where(mine, (within + carried).astype(I32) - low, -1)
    picked = jnp.zeros((SLOTS, hidden_ref.shape[2]), F32)
    for t in range(traces):
        hit = slot[t : t + 1, :] == iota((SLOTS, steps), 0)
        token = jnp.sum(jnp.where(hit, local[t : t + 1, :] + 1, 0).astype(F32), axis=1, keepdims=True)
        choose = jnp.where(token.astype(I32) == iota((SLOTS, tokens), 1) + 1, 1.0, 0.0).astype(BF16)
        picked += jnp.dot(choose, hidden_ref[t], preferred_element_type=F32)
    depth = hidden_ref.shape[2] // 2 // ZC
    half = hidden_ref.shape[2] // 2
    pad = jnp.zeros((SLOTS, 32 - depth), F32)
    for zc in range(ZC):
        parts = []
        for b in range(2):
            start = b * half + zc * depth
            parts += [picked[:, start : start + depth], pad]
        piece = jnp.concatenate(parts, axis=1)
        piece = jnp.concatenate([piece[: SLOTS // 2], piece[SLOTS // 2 :]], axis=1).astype(BF16)
        for x in range(NX):
            out_ref[x * ZC + zc] = piece


def layer_kernel(scalars, boundary_ref, picks_ref, weight_ref, out_ref):
    me, low, window = scalars[0], scalars[1], scalars[2]
    owner = boundary_ref[...] >> 6
    plane = me // ZC
    lane = iota((1, 128), 1)
    count = jnp.zeros((1, 128), F32)
    start = jnp.zeros((1, 128), F32)
    top = window.astype(F32)
    for zc in range(ZC):
        here = jnp.where(owner == plane * ZC + zc, 1.0, 0.0)
        number = jnp.sum(jnp.sum(here, axis=0, keepdims=True), axis=1, keepdims=True)
        number = jnp.clip(number - low.astype(F32), 0.0, top)
        count = count + jnp.where(lane // 8 == zc, number, 0.0)
        start = start + jnp.where(lane // 8 > zc, number, 0.0)
    count, start = count.astype(I32), start.astype(I32)
    choices = []
    for h in range(2):
        slot = lane % 8 + h * 8
        place = jnp.where(slot < count, start + slot, -1)
        choices.append(jnp.where(place == iota((CAP, 128), 0), 1.0, 0.0).astype(BF16))
    parts = []
    for x in range(NX):
        block = picks_ref[x * ZC : (x + 1) * ZC].reshape(ZC * 8, 128)
        left = jnp.dot(choices[0], block, preferred_element_type=F32)
        right = jnp.dot(choices[1], block, preferred_element_type=F32)
        parts.append(left[:, :64] + right[:, 64:])
    rows = jnp.concatenate(parts, axis=1).astype(BF16)
    weight = weight_ref[...].reshape(NY * 32, weight_ref.shape[2])
    partial = jnp.dot(rows, weight, preferred_element_type=F32)
    for h in range(2):
        for j in range(8):
            out_ref[h * 8 + j] = partial[h * HALF : (h + 1) * HALF, j * 128 : (j + 1) * 128]


def head_kernel(scalars, pre_ref, bias_ref, second_ref, out_ref):
    j = scalars[0] % 8
    pre = pre_ref[0]
    for zc in range(1, ZC):
        pre = pre + pre_ref[zc]
    unit = jnp.maximum(pre + bias_ref[pl.ds(j, 1), :], 0.0) * second_ref[pl.ds(j, 1), :]
    unit = jnp.concatenate([unit, jnp.zeros((128 - HALF, 128), F32)], axis=0)
    logit = lax.dot_general(
        jnp.ones((8, 128), F32), unit, (((1,), (1,)), ((), ())), precision=HIGH, preferred_element_type=F32
    )
    out_ref[...] = jnp.broadcast_to(logit[0:1, :].reshape(1, 1, 128), out_ref.shape)


def look_up_kernel(logit_ref, place_ref, out_ref):
    rows = []
    for y in range(NY):
        for h in range(2):
            first = y * ZC * NX + h * 8 * NX
            rows.append(jnp.sum(logit_ref[first : first + 8 * NX].reshape(8 * NX, 128), axis=0, keepdims=True))
    table = jnp.concatenate(rows, axis=0)
    place = place_ref[...]
    for t in range(place.shape[0]):
        row, lane = place[t : t + 1, :] // 128, place[t : t + 1, :] % 128
        spread = jnp.where(iota((128, place.shape[1]), 0) == lane, 1.0, 0.0)
        found = jnp.dot(table, spread, precision=HIGH, preferred_element_type=F32)
        found = jnp.where(iota(found.shape, 0) == row, found, 0.0)
        out_ref[t : t + 1, :] = jnp.sum(found, axis=0, keepdims=True)


def finish_kernel(logit_ref, valid_ref, pairs_ref, reward_ref, score_ref, margin_ref):
    logit = logit_ref[...]
    live = valid_ref[...] == 1
    reward_ref[...] = jnp.where(live, logit, 0.0)
    score = jnp.min(jnp.where(live, logit, 1e30), axis=1, keepdims=True)
    traces = logit.shape[0]
    diagonal = iota((traces, traces), 0) == iota((traces, traces), 1)
    flat = jnp.sum(jnp.where(diagonal, score, 0.0), axis=0, keepdims=True)
    score_ref[...] = flat
    trace = iota((traces, traces), 1)
    pairs = pairs_ref[...]
    ends = []
    for e in range(2):
        end = jnp.sum(jnp.where(pairs[:, e : e + 1] == trace, flat, 0.0), axis=1, keepdims=True)
        ends.append(end)
    margin_ref[...] = jnp.sum(jnp.where(diagonal, ends[0] - ends[1], 0.0), axis=0, keepdims=True)


def call(kernel, specs, shape, *args):
    single = not isinstance(shape, list)
    return pl.pallas_call(
        kernel,
        out_shape=shape,
        in_specs=specs,
        out_specs=VMEM if single else [VMEM] * len(shape),
        name=kernel.__name__,
    )(*args)


def exchange(pieces, axes):
    return lax.all_to_all(pieces, axes, split_axis=0, concat_axis=0, tiled=True)


def per_device(hidden_states, boundary, valid, pairs, w_first, b_first, w_second):
    columns = w_first.shape[1]
    me = lax.axis_index(SEQ).astype(I32)
    weight = jnp.pad(w_first, ((0, 32 - w_first.shape[0]), (0, 0)))
    weight = exchange(jnp.broadcast_to(weight, (NY, *weight.shape)), "y")
    bias, second = b_first.reshape(8, columns // 8), w_second.reshape(8, columns // 8)

    owner = (boundary >> 6).reshape(-1)
    order = jnp.arange(owner.shape[0], dtype=I32)
    same = owner[:, None] == owner[None, :]
    rank = jnp.sum(same & (order[None, :] < order[:, None]), axis=1, dtype=I32)
    most = jnp.max(rank) + 1
    plane = owner // ZC
    crowd = jnp.max(jnp.sum(plane[:, None] == plane[None, :], axis=1, dtype=I32))
    window = jnp.where((most <= SLOTS) & (crowd <= CAP), SLOTS, ROUND_SLOTS).astype(I32)

    def one_round(low, window):
        scalars = jnp.stack([me, low, window])
        picks = call(
            pick_kernel, [SMEM, VMEM, VMEM], jax.ShapeDtypeStruct((NX * ZC, 8, 128), BF16),
            scalars, boundary, hidden_states,
        )
        picks = exchange(picks, XZC)
        pre = call(
            layer_kernel, [SMEM, VMEM, VMEM, VMEM], jax.ShapeDtypeStruct((ZC, HALF, 128), F32),
            scalars, boundary, picks, weight,
        )
        pre = exchange(pre, ("z", "c"))
        share = call(
            head_kernel, [SMEM, VMEM, VMEM, VMEM], jax.ShapeDtypeStruct((NY * ZC * NX, 1, 128), F32),
            scalars, pre, bias, second,
        )
        share = exchange(share, ALL)
        inside = (rank >= low) & (rank < low + window)
        ahead = inside[None, :] & (plane[None, :] == plane[:, None]) & (owner[None, :] < owner[:, None])
        g = jnp.sum(ahead, axis=1, dtype=I32) + rank - low
        place = (plane * 2 + g // HALF) * 128 + g % HALF
        place = jnp.where(inside, place, -128).reshape(boundary.shape)
        return call(look_up_kernel, [VMEM, VMEM], jax.ShapeDtypeStruct(boundary.shape, F32), share, place)

    logit = one_round(jnp.int32(0), window)

    def more(state):
        low, total = state
        return low + ROUND_SLOTS, total + one_round(low, jnp.int32(ROUND_SLOTS))

    _, logit = lax.while_loop(lambda state: state[0] < most, more, (window, logit))
    reward, score, margin = call(
        finish_kernel, [VMEM] * 3,
        [jax.ShapeDtypeStruct(boundary.shape, F32)] + [jax.ShapeDtypeStruct((1, 8), F32)] * 2,
        logit, valid, pairs,
    )
    return reward, score.reshape(8), margin.reshape(8)


def solution(mesh):
    torus = Mesh(mesh.devices.reshape(NY, NZ, NC, NX), ALL)
    return jax.shard_map(
        per_device,
        mesh=torus,
        in_specs=(P(None, SEQ, "x"), P(), P(), P(), P(SEQ, "x"), P("x"), P("x")),
        out_specs=(P(), P(), P()),
        check_vma=False,
    )
```

```python
import jax
import jax.numpy as jnp
from jax import lax
from jax.experimental import pallas as pl
from jax.experimental.pallas import tpu as pltpu
from jax.sharding import Mesh
from jax.sharding import PartitionSpec as P

NYH, NY0, NZH, NZ0, NC, NX = 4, 2, 4, 2, 2, 4
NAMES = ("yh", "y0", "zh", "z0", "c", "x")
SEQ = NAMES[:5]
OWNERS = NYH * NY0 * NZ0 * NC
BLOCKS = NY0 * NZ0 * NC
SLOTS = 16
ROUND_SLOTS = 3
PART = 30
CAP = NX * PART
DEEP = 32
VMEM = pl.BlockSpec(memory_space=pltpu.VMEM)
SMEM = pl.BlockSpec(memory_space=pltpu.SMEM)
F32, BF16, I32 = jnp.float32, jnp.bfloat16, jnp.int32
HIGH = lax.Precision.HIGHEST


def iota(shape, dim):
    return lax.broadcasted_iota(I32, shape, dim)


def ones_where(test, dtype=F32):
    return jnp.where(test, 1.0, 0.0).astype(dtype)


def group_of(owner):
    return (owner >> 2) & 3


def pick_kernel(round_ref, boundary_ref, valid_ref, hidden_ref, out_ref):
    me, low = lax.axis_index(SEQ), round_ref[0]
    traces, steps = boundary_ref.shape
    tokens = hidden_ref.shape[1]
    local = boundary_ref[...] - me * tokens
    mine = (local >= 0) & (local < tokens) & (valid_ref[...] == 1)
    owned = ones_where(mine, BF16)
    before = ones_where(iota((steps, steps), 0) < iota((steps, steps), 1), BF16)
    within = jnp.dot(owned, before, preferred_element_type=F32)
    totals = jnp.dot(owned, jnp.ones((steps, steps), BF16), preferred_element_type=F32)
    earlier = ones_where(iota((traces, traces), 1) < iota((traces, traces), 0), BF16)
    carried = jnp.dot(earlier, totals.astype(BF16), preferred_element_type=F32)
    slot = jnp.where(mine, (within + carried).astype(I32) - low, -1)
    picked = jnp.zeros((SLOTS, hidden_ref.shape[2]), F32)
    for t in range(traces):
        hit = slot[t : t + 1, :] == iota((SLOTS, steps), 0)
        token = jnp.sum(jnp.where(hit, local[t : t + 1, :] + 1, 0).astype(F32), axis=1, keepdims=True)
        choose = ones_where(token.astype(I32) == iota((SLOTS, tokens), 1) + 1, BF16)
        picked += jnp.dot(choose, hidden_ref[t], preferred_element_type=F32)
    depth = hidden_ref.shape[2] // (BLOCKS * NZH)
    pad = jnp.zeros((SLOTS, DEEP - depth), F32)
    for y0 in range(NY0):
        for low2 in range(NZ0 * NC):
            parts = []
            for zh in range(NZH):
                start = (y0 * 16 + zh * 4 + low2) * depth
                parts += [picked[:, start : start + depth], pad]
            piece = jnp.concatenate(parts, axis=1).astype(BF16)
            for yh in range(NYH):
                out_ref[yh * BLOCKS + y0 * 4 + low2] = piece


def layer_kernel(round_ref, boundary_ref, valid_ref, picks_ref, weight_ref, bias_ref, second_ref, out_ref):
    low, window = round_ref[0], round_ref[1]
    traces, steps = boundary_ref.shape
    owner = jnp.where(valid_ref[...] == 1, boundary_ref[...] >> 6, -1)
    count = jnp.zeros((128, steps), F32)
    for t in range(traces):
        count += ones_where(owner[t : t + 1, :] == iota((128, steps), 0))
    count = jnp.sum(count, axis=1, keepdims=True)
    device = iota((128, 1), 0)
    most = jnp.max(count, axis=0, keepdims=True)
    fits = most <= SLOTS
    for zh in range(NZH):
        crowd = jnp.sum(jnp.where(group_of(device) == zh, count, 0.0), axis=0, keepdims=True)
        fits = fits & (crowd <= CAP)
    top = jnp.where(window > 0, window.astype(F32), jnp.where(fits, float(SLOTS), float(ROUND_SLOTS)))
    count = jnp.clip(count - low.astype(F32), 0.0, top)
    mine = group_of(device) == lax.axis_index("zh")
    count = jnp.where(mine, count, 0.0)
    place_in_group = (device >> 4) * 4 + (device & 3)
    lane = iota((128, OWNERS * SLOTS), 1) >> 4
    number = jnp.sum(jnp.where(lane == place_in_group, count, 0.0), axis=0, keepdims=True).astype(I32)
    start = jnp.sum(jnp.where(lane > place_in_group, count, 0.0), axis=0, keepdims=True).astype(I32)
    slot = iota((1, OWNERS * SLOTS), 1) & (SLOTS - 1)
    g = start + slot
    g = g + 2 * ((g >= PART).astype(I32) + (g >= 2 * PART).astype(I32) + (g >= 3 * PART).astype(I32))
    g = jnp.where(slot < number, g, -1)
    choose = ones_where(g == iota((NX * DEEP, OWNERS * SLOTS), 0), BF16)
    rows = jnp.dot(choose, picks_ref[...].reshape(OWNERS * SLOTS, 128), preferred_element_type=F32)
    weight = weight_ref[...].reshape(NZH * DEEP, weight_ref.shape[2])
    partial = jnp.dot(rows.astype(BF16), weight, preferred_element_type=F32)
    for x in range(NX):
        for j in range(BLOCKS):
            columns = slice(j * 128, (j + 1) * 128)
            out_ref[x * BLOCKS + j] = partial[x * DEEP : (x + 1) * DEEP, columns]
            out_ref[x * BLOCKS + j, PART : PART + 1, :] = bias_ref[j : j + 1, :]
            out_ref[x * BLOCKS + j, PART + 1 : PART + 2, :] = second_ref[j : j + 1, :]


def head_kernel(pre_ref, out_ref):
    pre = pre_ref[0]
    for source in range(1, NX * BLOCKS):
        pre = pre + pre_ref[source]
    extra = pre_ref[lax.axis_index("yh") * BLOCKS]
    unit = jnp.maximum(pre + extra[PART : PART + 1, :], 0.0) * extra[PART + 1 : PART + 2, :]
    unit = jnp.where(iota(unit.shape, 0) < PART, unit, 0.0)
    unit = jnp.concatenate([unit, jnp.zeros((128 - DEEP, 128), F32)], axis=0)
    logit = lax.dot_general(
        jnp.ones((8, 128), F32), unit, (((1,), (1,)), ((), ())), precision=HIGH, preferred_element_type=F32
    )
    out_ref[...] = jnp.broadcast_to(logit[0:1, :].reshape(1, 1, 128), out_ref.shape)


def finish_kernel(share_ref, place_ref, before_ref, valid_ref, pairs_ref, logit_ref, reward_ref, score_ref, margin_ref):
    each = share_ref.shape[0] // (NZH * NX)
    rows = []
    for group in range(NZH * NX):
        shares = share_ref[group * each : (group + 1) * each].reshape(each, 128)
        rows.append(jnp.sum(shares, axis=0, keepdims=True))
    table = jnp.concatenate(rows, axis=0)
    place = place_ref[...]
    traces, steps = place.shape
    logits = []
    for t in range(traces):
        row, lane = place[t : t + 1, :] >> 7, place[t : t + 1, :] & 127
        spread = ones_where(iota((128, steps), 0) == lane)
        found = jnp.dot(table, spread, precision=HIGH, preferred_element_type=F32)
        found = jnp.where(iota(found.shape, 0) == row, found, 0.0)
        logits.append(jnp.sum(found, axis=0, keepdims=True))
    logit = before_ref[...] + jnp.concatenate(logits, axis=0)
    logit_ref[...] = logit
    live = valid_ref[...] == 1
    reward_ref[...] = jnp.where(live, logit, 0.0)
    score = jnp.min(jnp.where(live, logit, 1e30), axis=1, keepdims=True)
    diagonal = iota((traces, traces), 0) == iota((traces, traces), 1)
    flat = jnp.sum(jnp.where(diagonal, score, 0.0), axis=0, keepdims=True)
    score_ref[...] = flat
    trace = iota((traces, traces), 1)
    pairs = pairs_ref[...]
    ends = []
    for e in range(2):
        ends.append(jnp.sum(jnp.where(pairs[:, e : e + 1] == trace, flat, 0.0), axis=1, keepdims=True))
    margin_ref[...] = jnp.sum(jnp.where(diagonal, ends[0] - ends[1], 0.0), axis=0, keepdims=True)


def call(kernel, shapes, *args, scalars=0):
    single = not isinstance(shapes, list)
    return pl.pallas_call(
        kernel,
        out_shape=shapes,
        in_specs=[SMEM] * scalars + [VMEM] * (len(args) - scalars),
        out_specs=VMEM if single else [VMEM] * len(shapes),
        compiler_params=pltpu.CompilerParams(vmem_limit_bytes=16 << 20),
        name=kernel.__name__,
    )(*args)


def array(shape, dtype=F32):
    return jax.ShapeDtypeStruct(shape, dtype)


def exchange(pieces, axes):
    return lax.all_to_all(pieces, axes, split_axis=0, concat_axis=0, tiled=True)


def per_device(hidden_states, boundary, valid, pairs, w_first, b_first, w_second):
    columns = w_first.shape[1]
    weight = jnp.pad(w_first, ((0, DEEP - w_first.shape[0]), (0, 0)))
    swap = [(a * NX + b, b * NX + a) for a in range(NYH) for b in range(NX)]
    weight = lax.ppermute(weight, ("yh", "x"), swap)
    weight = lax.all_gather(weight, "zh")
    bias, second = b_first.reshape(8, columns // 8), w_second.reshape(8, columns // 8)

    owner = (boundary >> 6).reshape(-1)
    live = valid.reshape(-1) == 1
    order = jnp.arange(owner.shape[0], dtype=I32)
    same = (owner[:, None] == owner[None, :]) & live[None, :]
    rank = jnp.sum(same & (order[None, :] < order[:, None]), axis=1, dtype=I32)
    most = jnp.max(jnp.where(live, rank + 1, 0))
    group = group_of(owner)
    crowd = jnp.max(jnp.sum((group[:, None] == group[None, :]) & live[None, :], axis=1, dtype=I32))
    first_window = jnp.where((most <= SLOTS) & (crowd <= CAP), SLOTS, ROUND_SLOTS).astype(I32)

    def one_round(numbers, low, window, before):
        picks = call(
            pick_kernel, array((OWNERS, SLOTS, 128), BF16), numbers, boundary, valid, hidden_states, scalars=1
        )
        picks = exchange(picks, ("yh", "y0", "z0", "c"))
        pre = call(
            layer_kernel, array((NX * BLOCKS, DEEP, 128)),
            numbers, boundary, valid, picks, weight, bias, second, scalars=1,
        )
        pre = exchange(pre, ("x", "y0", "z0", "c"))
        share = call(head_kernel, array((NYH * NX * BLOCKS * NZH, 1, 128)), pre)
        share = exchange(share, ("zh", "x", "yh", "y0", "z0", "c"))
        inside = live & (rank >= low) & (rank < low + window)
        ahead = inside[None, :] & (group[None, :] == group[:, None]) & (owner[None, :] < owner[:, None])
        g = jnp.sum(ahead, axis=1, dtype=I32) + rank - low
        place = (group * NX + g // PART) * 128 + g % PART
        place = jnp.where(inside, place, -128).reshape(boundary.shape)
        return call(
            finish_kernel, [array(boundary.shape), array(boundary.shape), array((1, 8)), array((1, 8))],
            share, place, before, valid, pairs,
        )

    first = jnp.array([0, 0], I32)
    found = one_round(first, 0, first_window, jnp.zeros(boundary.shape, F32))

    def more(state):
        low, found = state
        numbers = jnp.stack([low, jnp.int32(ROUND_SLOTS)])
        return low + ROUND_SLOTS, one_round(numbers, low, ROUND_SLOTS, found[0])

    _, found = lax.while_loop(lambda state: state[0] < most, more, (first_window, found))
    return found[1], found[2].reshape(8), found[3].reshape(8)


def solution(mesh):
    torus = Mesh(mesh.devices.reshape(NYH, NY0, NZH, NZ0, NC, NX), NAMES)
    return jax.shard_map(
        per_device,
        mesh=torus,
        in_specs=(P(None, SEQ, "x"), P(), P(), P(), P(SEQ, "x"), P("x"), P("x")),
        out_specs=(P(), P(), P()),
        check_vma=False,
    )
```

```python
import jax
import jax.numpy as jnp
from jax import lax
from jax.experimental import pallas as pl
from jax.experimental.pallas import tpu as pltpu
from jax.sharding import Mesh
from jax.sharding import PartitionSpec as P

NYH, NY0, NZH, NZ0, NC, NX = 4, 2, 4, 2, 2, 4
NAMES = ("yh", "y0", "zh", "z0", "c", "x")
SEQ = NAMES[:5]
OWNERS = NYH * NY0 * NZ0 * NC
BLOCKS = NY0 * NZ0 * NC
SLOTS = 16
ROUND_SLOTS = 3
PART = 30
CAP = NX * PART
DEEP = 32
VMEM = pl.BlockSpec(memory_space=pltpu.VMEM)
SMEM = pl.BlockSpec(memory_space=pltpu.SMEM)
F32, BF16, I32 = jnp.float32, jnp.bfloat16, jnp.int32
HIGH = lax.Precision.HIGHEST


def iota(shape, dim):
    return lax.broadcasted_iota(I32, shape, dim)


def ones_where(test, dtype=F32):
    return jnp.where(test, 1.0, 0.0).astype(dtype)


def group_of(owner):
    return (owner >> 2) & 3


def first_pick_kernel(round_ref, boundary_ref, valid_ref, hidden_ref, bias_ref, second_ref, out_ref, extra_ref):
    extra_ref[0] = bias_ref[...]
    extra_ref[1] = second_ref[...]
    pick_kernel(round_ref, boundary_ref, valid_ref, hidden_ref, out_ref)


def pick_kernel(round_ref, boundary_ref, valid_ref, hidden_ref, out_ref):
    me, low = lax.axis_index(SEQ), round_ref[0]
    traces, steps = boundary_ref.shape
    tokens = hidden_ref.shape[1]
    local = boundary_ref[...] - me * tokens
    mine = (local >= 0) & (local < tokens) & (valid_ref[...] == 1)
    owned = ones_where(mine, BF16)
    before = ones_where(iota((steps, steps), 0) < iota((steps, steps), 1), BF16)
    within = jnp.dot(owned, before, preferred_element_type=F32)
    totals = jnp.dot(owned, jnp.ones((steps, steps), BF16), preferred_element_type=F32)
    earlier = ones_where(iota((traces, traces), 1) < iota((traces, traces), 0), BF16)
    carried = jnp.dot(earlier, totals.astype(BF16), preferred_element_type=F32)
    slot = jnp.where(mine, (within + carried).astype(I32) - low, -1)
    picked = jnp.zeros((SLOTS, hidden_ref.shape[2]), F32)
    for t in range(traces):
        hit = slot[t : t + 1, :] == iota((SLOTS, steps), 0)
        token = jnp.sum(jnp.where(hit, local[t : t + 1, :] + 1, 0).astype(F32), axis=1, keepdims=True)
        choose = ones_where(token.astype(I32) == iota((SLOTS, tokens), 1) + 1, BF16)
        picked += jnp.dot(choose, hidden_ref[t], preferred_element_type=F32)
    depth = hidden_ref.shape[2] // (BLOCKS * NZH)
    pad = jnp.zeros((SLOTS, DEEP - depth), F32)
    for y0 in range(NY0):
        for low2 in range(NZ0 * NC):
            parts = []
            for zh in (0, 3, 2, 1):
                start = (y0 * 16 + zh * 4 + low2) * depth
                parts += [picked[:, start : start + depth], pad]
            piece = jnp.concatenate(parts, axis=1).astype(BF16)
            for yh in range(NYH):
                out_ref[yh * BLOCKS + y0 * 4 + low2] = piece


def layer_kernel(round_ref, boundary_ref, valid_ref, picks_ref, extra_ref, w0_ref, w1_ref, w2_ref, w3_ref, out_ref):
    low, window = round_ref[0], round_ref[1]
    traces, steps = boundary_ref.shape
    owner = jnp.where(valid_ref[...] == 1, boundary_ref[...] >> 6, -1)
    count = jnp.zeros((128, steps), F32)
    for t in range(traces):
        count += ones_where(owner[t : t + 1, :] == iota((128, steps), 0))
    count = jnp.sum(count, axis=1, keepdims=True)
    device = iota((128, 1), 0)
    most = jnp.max(count, axis=0, keepdims=True)
    fits = most <= SLOTS
    for group in range(NZH):
        crowd = jnp.sum(jnp.where(group_of(device) == group, count, 0.0), axis=0, keepdims=True)
        fits = fits & (crowd <= CAP)
    top = jnp.where(window > 0, window.astype(F32), jnp.where(fits, float(SLOTS), float(ROUND_SLOTS)))
    count = jnp.clip(count - low.astype(F32), 0.0, top)
    zh = lax.axis_index("zh")
    mine = group_of(device) == zh
    count = jnp.where(mine, count, 0.0)
    place_in_group = (device >> 4) * 4 + (device & 3)
    lane = iota((128, OWNERS * SLOTS), 1) >> 4
    number = jnp.sum(jnp.where(lane == place_in_group, count, 0.0), axis=0, keepdims=True).astype(I32)
    start = jnp.sum(jnp.where(lane > place_in_group, count, 0.0), axis=0, keepdims=True).astype(I32)
    slot = iota((1, OWNERS * SLOTS), 1) & (SLOTS - 1)
    g = start + slot
    g = g + 2 * ((g >= PART).astype(I32) + (g >= 2 * PART).astype(I32) + (g >= 3 * PART).astype(I32))
    g = jnp.where(slot < number, g, -1)
    choose = ones_where(g == iota((NX * DEEP, OWNERS * SLOTS), 0), BF16)
    rows = jnp.dot(choose, picks_ref[...].reshape(OWNERS * SLOTS, 128), preferred_element_type=F32)
    rows = pltpu.roll(rows, zh * DEEP, 1)
    pad = jnp.zeros((DEEP - w0_ref.shape[0], w0_ref.shape[1]), BF16)
    weight = []
    for ref in (w0_ref, w1_ref, w2_ref, w3_ref):
        weight += [ref[...], pad]
    partial = jnp.dot(rows.astype(BF16), jnp.concatenate(weight, axis=0), preferred_element_type=F32)
    for x in range(NX):
        for j in range(BLOCKS):
            columns = slice(j * 128, (j + 1) * 128)
            out_ref[x * BLOCKS + j] = partial[x * DEEP : (x + 1) * DEEP, columns]
            out_ref[x * BLOCKS + j, PART : PART + 1, :] = extra_ref[0, j : j + 1, :]
            out_ref[x * BLOCKS + j, PART + 1 : PART + 2, :] = extra_ref[1, j : j + 1, :]


def head_kernel(pre_ref, out_ref):
    pre = pre_ref[0]
    for source in range(1, NX * BLOCKS):
        pre = pre + pre_ref[source]
    extra = pre_ref[lax.rem(lax.axis_index("yh") + 2, NX) * BLOCKS]
    unit = jnp.maximum(pre + extra[PART : PART + 1, :], 0.0) * extra[PART + 1 : PART + 2, :]
    unit = jnp.where(iota(unit.shape, 0) < PART, unit, 0.0)
    unit = jnp.concatenate([unit, jnp.zeros((128 - DEEP, 128), F32)], axis=0)
    logit = lax.dot_general(
        jnp.ones((8, 128), F32), unit, (((1,), (1,)), ((), ())), precision=HIGH, preferred_element_type=F32
    )
    out_ref[...] = jnp.broadcast_to(logit[0:1, :].reshape(1, 1, 128), out_ref.shape)


def spread_kernel(share_ref, out_ref):
    out_ref[...] = jnp.broadcast_to(jnp.sum(share_ref[...], axis=0, keepdims=True), out_ref.shape)


def finish_kernel(share_ref, place_ref, before_ref, valid_ref, pairs_ref, logit_ref, reward_ref, score_ref, margin_ref):
    each = share_ref.shape[0] // (NZH * NX)
    rows = []
    for group in range(NZH * NX):
        shares = share_ref[group * each : (group + 1) * each].reshape(each, 128)
        rows.append(jnp.sum(shares, axis=0, keepdims=True))
    table = jnp.concatenate(rows, axis=0)
    place = place_ref[...]
    traces, steps = place.shape
    logits = []
    for t in range(traces):
        row, lane = place[t : t + 1, :] >> 7, place[t : t + 1, :] & 127
        spread = ones_where(iota((128, steps), 0) == lane)
        found = jnp.dot(table, spread, precision=HIGH, preferred_element_type=F32)
        found = jnp.where(iota(found.shape, 0) == row, found, 0.0)
        logits.append(jnp.sum(found, axis=0, keepdims=True))
    logit = before_ref[...] + jnp.concatenate(logits, axis=0)
    logit_ref[...] = logit
    live = valid_ref[...] == 1
    reward_ref[...] = jnp.where(live, logit, 0.0)
    score = jnp.min(jnp.where(live, logit, 1e30), axis=1, keepdims=True)
    diagonal = iota((traces, traces), 0) == iota((traces, traces), 1)
    flat = jnp.sum(jnp.where(diagonal, score, 0.0), axis=0, keepdims=True)
    score_ref[...] = flat
    trace = iota((traces, traces), 1)
    pairs = pairs_ref[...]
    ends = []
    for e in range(2):
        ends.append(jnp.sum(jnp.where(pairs[:, e : e + 1] == trace, flat, 0.0), axis=1, keepdims=True))
    margin_ref[...] = jnp.sum(jnp.where(diagonal, ends[0] - ends[1], 0.0), axis=0, keepdims=True)


def call(kernel, shapes, *args, scalars=0):
    single = not isinstance(shapes, list)
    return pl.pallas_call(
        kernel,
        out_shape=shapes,
        in_specs=[SMEM] * scalars + [VMEM] * (len(args) - scalars),
        out_specs=VMEM if single else [VMEM] * len(shapes),
        compiler_params=pltpu.CompilerParams(vmem_limit_bytes=16 << 20),
        name=kernel.__name__,
    )(*args)


def array(shape, dtype=F32):
    return jax.ShapeDtypeStruct(shape, dtype)


def exchange(pieces, axes):
    return lax.all_to_all(pieces, axes, split_axis=0, concat_axis=0, tiled=True)


def per_device(hidden_states, boundary, valid, pairs, w_first, b_first, w_second):
    columns = w_first.shape[1]
    swap = [(a * NX + b, (b + 2) % NYH * NX + a) for a in range(NYH) for b in range(NX)]
    weights = [lax.ppermute(w_first, ("yh", "x"), swap)]
    for k in range(1, NZH):
        weights.append(lax.ppermute(weights[0], "zh", [(i, (i + k) % NZH) for i in range(NZH)]))
    bias, second = b_first.reshape(8, columns // 8), w_second.reshape(8, columns // 8)

    owner = (boundary >> 6).reshape(-1)
    live = valid.reshape(-1) == 1
    order = jnp.arange(owner.shape[0], dtype=I32)
    same = (owner[:, None] == owner[None, :]) & live[None, :]
    rank = jnp.sum(same & (order[None, :] < order[:, None]), axis=1, dtype=I32)
    most = jnp.max(jnp.where(live, rank + 1, 0))
    group = group_of(owner)
    crowd = jnp.max(jnp.sum((group[:, None] == group[None, :]) & live[None, :], axis=1, dtype=I32))
    first_window = jnp.where((most <= SLOTS) & (crowd <= CAP), SLOTS, ROUND_SLOTS).astype(I32)

    shape = array((OWNERS, SLOTS, 128), BF16)

    def one_round(numbers, low, window, before, picks, extra):
        picks = exchange(picks, ("yh", "y0", "z0", "c"))
        pre = call(
            layer_kernel, array((NX * BLOCKS, DEEP, 128)),
            numbers, boundary, valid, picks, extra, *weights, scalars=1,
        )
        pre = exchange(pre, ("x", "y0", "z0", "c"))
        share = exchange(call(head_kernel, array((NYH * NY0, 1, 128)), pre), ("yh", "y0"))
        share = call(spread_kernel, array((NZH * NX * NZ0 * NC, 1, 128)), share)
        share = exchange(share, ("zh", "x", "z0", "c"))
        inside = live & (rank >= low) & (rank < low + window)
        ahead = inside[None, :] & (group[None, :] == group[:, None]) & (owner[None, :] < owner[:, None])
        g = jnp.sum(ahead, axis=1, dtype=I32) + rank - low
        place = (group * NX + g // PART) * 128 + g % PART
        place = jnp.where(inside, place, -128).reshape(boundary.shape)
        return call(
            finish_kernel, [array(boundary.shape), array(boundary.shape), array((1, 8)), array((1, 8))],
            share, place, before, valid, pairs,
        )

    first = jnp.array([0, 0], I32)
    picks, extra = call(
        first_pick_kernel, [shape, array((2, 8, 128))],
        first, boundary, valid, hidden_states, bias, second, scalars=1,
    )
    found = one_round(first, 0, first_window, jnp.zeros(boundary.shape, F32), picks, extra)

    def more(state):
        low, found = state
        numbers = jnp.stack([low, jnp.int32(ROUND_SLOTS)])
        picks = call(pick_kernel, shape, numbers, boundary, valid, hidden_states, scalars=1)
        return low + ROUND_SLOTS, one_round(numbers, low, ROUND_SLOTS, found[0], picks, extra)

    _, found = lax.while_loop(lambda state: state[0] < most, more, (first_window, found))
    return found[1], found[2].reshape(8), found[3].reshape(8)


def solution(mesh):
    torus = Mesh(mesh.devices.reshape(NYH, NY0, NZH, NZ0, NC, NX), NAMES)
    return jax.shard_map(
        per_device,
        mesh=torus,
        in_specs=(P(None, SEQ, "x"), P(), P(), P(), P(SEQ, "x"), P("x"), P("x")),
        out_specs=(P(), P(), P()),
        check_vma=False,
    )
```

```python
import jax
import jax.numpy as jnp
from jax import lax
from jax.experimental import pallas as pl
from jax.experimental.pallas import tpu as pltpu
from jax.sharding import Mesh
from jax.sharding import PartitionSpec as P

NYH, NY0, NZH, NZ0, NC, NX = 4, 2, 4, 2, 2, 4
NAMES = ("yh", "y0", "z2", "z1", "z0", "c", "x")
SEQ = NAMES[:6]
ZH = ("z2", "z1")
OWNERS = NYH * NY0 * NZ0 * NC
BLOCKS = NY0 * NZ0 * NC
SLOTS = 16
ROUND_SLOTS = 3
PART = 30
CAP = NX * PART
DEEP = 32
VMEM = pl.BlockSpec(memory_space=pltpu.VMEM)
SMEM = pl.BlockSpec(memory_space=pltpu.SMEM)
F32, BF16, I32 = jnp.float32, jnp.bfloat16, jnp.int32
HIGH = lax.Precision.HIGHEST


def iota(shape, dim):
    return lax.broadcasted_iota(I32, shape, dim)


def ones_where(test, dtype=F32):
    return jnp.where(test, 1.0, 0.0).astype(dtype)


def group_of(owner):
    return (owner >> 2) & 3


def first_pick_kernel(round_ref, boundary_ref, valid_ref, hidden_ref, bias_ref, second_ref, out_ref, extra_ref):
    extra_ref[0] = bias_ref[...]
    extra_ref[1] = second_ref[...]
    pick_kernel(round_ref, boundary_ref, valid_ref, hidden_ref, out_ref)


def pick_kernel(round_ref, boundary_ref, valid_ref, hidden_ref, out_ref):
    me, low = lax.axis_index(SEQ), round_ref[0]
    traces, steps = boundary_ref.shape
    tokens = hidden_ref.shape[1]
    local = boundary_ref[...] - me * tokens
    mine = (local >= 0) & (local < tokens) & (valid_ref[...] == 1)
    owned = ones_where(mine, BF16)
    before = ones_where(iota((steps, steps), 0) < iota((steps, steps), 1), BF16)
    within = jnp.dot(owned, before, preferred_element_type=F32)
    totals = jnp.dot(owned, jnp.ones((steps, steps), BF16), preferred_element_type=F32)
    earlier = ones_where(iota((traces, traces), 1) < iota((traces, traces), 0), BF16)
    carried = jnp.dot(earlier, totals.astype(BF16), preferred_element_type=F32)
    slot = jnp.where(mine, (within + carried).astype(I32) - low, -1)
    picked = jnp.zeros((SLOTS, hidden_ref.shape[2]), F32)
    for t in range(traces):
        hit = slot[t : t + 1, :] == iota((SLOTS, steps), 0)
        token = jnp.sum(jnp.where(hit, local[t : t + 1, :] + 1, 0).astype(F32), axis=1, keepdims=True)
        choose = ones_where(token.astype(I32) == iota((SLOTS, tokens), 1) + 1, BF16)
        picked += jnp.dot(choose, hidden_ref[t], preferred_element_type=F32)
    depth = hidden_ref.shape[2] // (BLOCKS * NZH)
    pad = jnp.zeros((SLOTS, DEEP - depth), F32)
    for y0 in range(NY0):
        for low2 in range(NZ0 * NC):
            parts = []
            for zh in range(NZH):
                start = (y0 * 16 + zh * 4 + low2) * depth
                parts += [picked[:, start : start + depth], pad]
            piece = jnp.concatenate(parts, axis=1).astype(BF16)
            for yh in range(NYH):
                out_ref[yh * BLOCKS + y0 * 4 + low2] = piece


def layer_kernel(round_ref, boundary_ref, valid_ref, picks_ref, extra_ref, weight_ref, out_ref):
    low, window = round_ref[0], round_ref[1]
    traces, steps = boundary_ref.shape
    owner = jnp.where(valid_ref[...] == 1, boundary_ref[...] >> 6, -1)
    count = jnp.zeros((128, steps), F32)
    for t in range(traces):
        count += ones_where(owner[t : t + 1, :] == iota((128, steps), 0))
    count = jnp.sum(count, axis=1, keepdims=True)
    device = iota((128, 1), 0)
    most = jnp.max(count, axis=0, keepdims=True)
    fits = most <= SLOTS
    for group in range(NZH):
        crowd = jnp.sum(jnp.where(group_of(device) == group, count, 0.0), axis=0, keepdims=True)
        fits = fits & (crowd <= CAP)
    top = jnp.where(window > 0, window.astype(F32), jnp.where(fits, float(SLOTS), float(ROUND_SLOTS)))
    count = jnp.clip(count - low.astype(F32), 0.0, top)
    zh = lax.axis_index(ZH)
    mine = group_of(device) == zh
    count = jnp.where(mine, count, 0.0)
    place_in_group = (device >> 4) * 4 + (device & 3)
    lane = iota((128, OWNERS * SLOTS), 1) >> 4
    number = jnp.sum(jnp.where(lane == place_in_group, count, 0.0), axis=0, keepdims=True).astype(I32)
    start = jnp.sum(jnp.where(lane > place_in_group, count, 0.0), axis=0, keepdims=True).astype(I32)
    slot = iota((1, OWNERS * SLOTS), 1) & (SLOTS - 1)
    g = start + slot
    g = g + 2 * ((g >= PART).astype(I32) + (g >= 2 * PART).astype(I32) + (g >= 3 * PART).astype(I32))
    g = jnp.where(slot < number, g, -1)
    choose = ones_where(g == iota((NX * DEEP, OWNERS * SLOTS), 0), BF16)
    rows = jnp.dot(choose, picks_ref[...].reshape(OWNERS * SLOTS, 128), preferred_element_type=F32)
    pad = jnp.zeros((DEEP - weight_ref.shape[1], weight_ref.shape[2]), BF16)
    weight = []
    for source in range(NZH):
        weight += [weight_ref[(source & 1) * 2 + ((source >> 1) ^ (zh >> 1))], pad]
    partial = jnp.dot(rows.astype(BF16), jnp.concatenate(weight, axis=0), preferred_element_type=F32)
    for x in range(NX):
        for j in range(BLOCKS):
            columns = slice(j * 128, (j + 1) * 128)
            out_ref[x * BLOCKS + j] = partial[x * DEEP : (x + 1) * DEEP, columns]
            out_ref[x * BLOCKS + j, PART : PART + 1, :] = extra_ref[0, j : j + 1, :]
            out_ref[x * BLOCKS + j, PART + 1 : PART + 2, :] = extra_ref[1, j : j + 1, :]


def head_kernel(pre_ref, out_ref):
    pre = pre_ref[0]
    for source in range(1, NX * BLOCKS):
        pre = pre + pre_ref[source]
    extra = pre_ref[lax.axis_index("yh") * BLOCKS]
    unit = jnp.maximum(pre + extra[PART : PART + 1, :], 0.0) * extra[PART + 1 : PART + 2, :]
    unit = jnp.where(iota(unit.shape, 0) < PART, unit, 0.0)
    unit = jnp.concatenate([unit, jnp.zeros((128 - DEEP, 128), F32)], axis=0)
    logit = lax.dot_general(
        jnp.ones((8, 128), F32), unit, (((1,), (1,)), ((), ())), precision=HIGH, preferred_element_type=F32
    )
    out_ref[...] = jnp.broadcast_to(logit[0:1, :].reshape(1, 1, 128), out_ref.shape)


def spread_kernel(share_ref, out_ref):
    out_ref[...] = jnp.broadcast_to(jnp.sum(share_ref[...], axis=0, keepdims=True), out_ref.shape)


def finish_kernel(share_ref, place_ref, before_ref, valid_ref, pairs_ref, logit_ref, reward_ref, score_ref, margin_ref):
    each = share_ref.shape[0] // (NZH * NX)
    rows = []
    for group in range(NZH * NX):
        shares = share_ref[group * each : (group + 1) * each].reshape(each, 128)
        rows.append(jnp.sum(shares, axis=0, keepdims=True))
    place = place_ref[...]
    traces, steps = valid_ref.shape
    row, lane = place >> 7, place & 127
    found = jnp.zeros(place.shape, F32)
    for group in range(NZH * NX):
        here = jnp.take_along_axis(jnp.broadcast_to(rows[group], place.shape), lane, axis=1)
        found = jnp.where(row == group, here, found)
    logit = before_ref[...] + found[:, :steps]
    logit_ref[...] = logit
    live = valid_ref[...] == 1
    reward_ref[...] = jnp.where(live, logit, 0.0)
    score = jnp.min(jnp.where(live, logit, 1e30), axis=1, keepdims=True)
    diagonal = iota((traces, traces), 0) == iota((traces, traces), 1)
    flat = jnp.sum(jnp.where(diagonal, score, 0.0), axis=0, keepdims=True)
    score_ref[...] = flat
    trace = iota((traces, traces), 1)
    pairs = pairs_ref[...]
    ends = []
    for e in range(2):
        ends.append(jnp.sum(jnp.where(pairs[:, e : e + 1] == trace, flat, 0.0), axis=1, keepdims=True))
    margin_ref[...] = jnp.sum(jnp.where(diagonal, ends[0] - ends[1], 0.0), axis=0, keepdims=True)


def call(kernel, shapes, *args, scalars=0):
    single = not isinstance(shapes, list)
    return pl.pallas_call(
        kernel,
        out_shape=shapes,
        in_specs=[SMEM] * scalars + [VMEM] * (len(args) - scalars),
        out_specs=VMEM if single else [VMEM] * len(shapes),
        compiler_params=pltpu.CompilerParams(vmem_limit_bytes=16 << 20),
        name=kernel.__name__,
    )(*args)


def array(shape, dtype=F32):
    return jax.ShapeDtypeStruct(shape, dtype)


def exchange(pieces, axes):
    return lax.all_to_all(pieces, axes, split_axis=0, concat_axis=0, tiled=True)


def per_device(hidden_states, boundary, valid, pairs, w_first, b_first, w_second):
    columns = w_first.shape[1]
    weights = []
    for flip in range(2):
        swap = []
        for a in range(NYH):
            for z in range(2):
                swap += [((a * 2 + z) * NX + b, (b * 2 + (z ^ flip)) * NX + a) for b in range(NX)]
        weights.append(lax.ppermute(w_first, ("yh", "z2", "x"), swap))
    weight = lax.all_gather(jnp.stack(weights), "z1").reshape(NZH, *w_first.shape)
    bias, second = b_first.reshape(8, columns // 8), w_second.reshape(8, columns // 8)

    def ranks(boundary, valid):
        owner = (boundary >> 6).reshape(-1)
        live = valid.reshape(-1) == 1
        order = jnp.arange(owner.shape[0], dtype=I32)
        same = (owner[:, None] == owner[None, :]) & live[None, :]
        rank = jnp.sum(same & (order[None, :] < order[:, None]), axis=1, dtype=I32)
        return owner, live, rank, group_of(owner)

    def limits(owner, live, rank, group):
        most = jnp.max(jnp.where(live, rank + 1, 0))
        crowd = jnp.max(jnp.sum((group[:, None] == group[None, :]) & live[None, :], axis=1, dtype=I32))
        return most, jnp.where((most <= SLOTS) & (crowd <= CAP), SLOTS, ROUND_SLOTS).astype(I32)

    shape = array((OWNERS, SLOTS, 128), BF16)

    def one_round(numbers, low, window, before, picks, extra):
        most = None
        picks = exchange(picks, ("yh", "y0", "z0", "c"))
        pre = call(
            layer_kernel, array((NX * BLOCKS, DEEP, 128)),
            numbers, boundary, valid, picks, extra, weight, scalars=1,
        )
        pre, late_boundary, late_valid = lax.optimization_barrier((pre, boundary, valid))
        owner, live, rank, group = ranks(late_boundary, late_valid)
        if window is None:
            most, window = limits(owner, live, rank, group)
        pre = exchange(pre, ("x", "y0", "z0", "c"))
        share = exchange(call(head_kernel, array((NYH * NY0 * NC, 1, 128)), pre), ("yh", "y0", "c"))
        share = call(spread_kernel, array((NZH * NX * NZ0, 1, 128)), share)
        share = exchange(share, ZH + ("x", "z0"))
        inside = live & (rank >= low) & (rank < low + window)
        ahead = inside[None, :] & (group[None, :] == group[:, None]) & (owner[None, :] < owner[:, None])
        g = jnp.sum(ahead, axis=1, dtype=I32) + rank - low
        place = (group * NX + g // PART) * 128 + g % PART
        place = jnp.where(inside, place, -128).reshape(boundary.shape)
        place = jnp.pad(place, ((0, 0), (0, 128 - boundary.shape[1])), constant_values=-128)
        found = call(
            finish_kernel, [array(boundary.shape), array(boundary.shape), array((1, 8)), array((1, 8))],
            share, place, before, valid, pairs,
        )
        return found, most, window

    first = jnp.array([0, 0], I32)
    picks, extra = call(
        first_pick_kernel, [shape, array((2, 8, 128))],
        first, boundary, valid, hidden_states, bias, second, scalars=1,
    )
    found, most, window = one_round(first, 0, None, jnp.zeros(boundary.shape, F32), picks, extra)

    def more(state):
        low, found = state
        numbers = jnp.stack([low, jnp.int32(ROUND_SLOTS)])
        picks = call(pick_kernel, shape, numbers, boundary, valid, hidden_states, scalars=1)
        found, _, _ = one_round(numbers, low, ROUND_SLOTS, found[0], picks, extra)
        return low + ROUND_SLOTS, found

    _, found = lax.while_loop(lambda state: state[0] < most, more, (window, found))
    return found[1], found[2].reshape(8), found[3].reshape(8)


def solution(mesh):
    torus = Mesh(mesh.devices.reshape(NYH, NY0, 2, 2, NZ0, NC, NX), NAMES)
    return jax.shard_map(
        per_device,
        mesh=torus,
        in_specs=(P(None, SEQ, "x"), P(), P(), P(), P(SEQ, "x"), P("x"), P("x")),
        out_specs=(P(), P(), P()),
        check_vma=False,
    )
```

```python
import jax
import jax.numpy as jnp
from jax import lax
from jax.experimental import pallas as pl
from jax.experimental.pallas import tpu as pltpu
from jax.sharding import Mesh
from jax.sharding import PartitionSpec as P

NYH, NY0, NZH, NZ0, NC, NX = 4, 2, 4, 2, 2, 4
NAMES = ("yh", "y0", "z2", "z1", "z0", "c", "x")
SEQ = NAMES[:6]
ZH = ("z2", "z1")
OWNERS = NYH * NY0 * NZ0 * NC
BLOCKS = NY0 * NZ0 * NC
SLOTS = 16
ROUND_SLOTS = 3
PART = 30
CAP = NX * PART
DEEP = 32
VMEM = pl.BlockSpec(memory_space=pltpu.VMEM)
SMEM = pl.BlockSpec(memory_space=pltpu.SMEM)
F32, BF16, I32 = jnp.float32, jnp.bfloat16, jnp.int32
HIGH = lax.Precision.HIGHEST


def iota(shape, dim):
    return lax.broadcasted_iota(I32, shape, dim)


def ones_where(test, dtype=F32):
    return jnp.where(test, 1.0, 0.0).astype(dtype)


def group_of(owner):
    return (owner >> 2) & 3


def first_pick_kernel(
    round_ref, boundary_ref, valid_ref, far_ref, bias_ref, second_ref, out_ref, extra_ref, hidden_ref, sems
):
    copies = [
        pltpu.make_async_copy(bias_ref, extra_ref.at[0], sems.at[1]),
        pltpu.make_async_copy(second_ref, extra_ref.at[1], sems.at[2]),
    ]
    pick_kernel(round_ref, boundary_ref, valid_ref, far_ref, out_ref, hidden_ref, sems, copies)


def pick_kernel(round_ref, boundary_ref, valid_ref, far_ref, out_ref, hidden_ref, sems, others=()):
    copies = [pltpu.make_async_copy(far_ref, hidden_ref, sems.at[0]), *others]
    for copy in copies:
        copy.start()
    me, low = lax.axis_index(SEQ), round_ref[0]
    traces, steps = boundary_ref.shape
    tokens = hidden_ref.shape[1]
    local = boundary_ref[...] - me * tokens
    mine = (local >= 0) & (local < tokens) & (valid_ref[...] == 1)
    owned = ones_where(mine, BF16)
    before = ones_where(iota((steps, steps), 0) < iota((steps, steps), 1), BF16)
    within = jnp.dot(owned, before, preferred_element_type=F32)
    totals = jnp.dot(owned, jnp.ones((steps, steps), BF16), preferred_element_type=F32)
    earlier = ones_where(iota((traces, traces), 1) < iota((traces, traces), 0), BF16)
    carried = jnp.dot(earlier, totals.astype(BF16), preferred_element_type=F32)
    slot = jnp.where(mine, (within + carried).astype(I32) - low, -1)
    chosen = []
    for t in range(traces):
        hit = slot[t : t + 1, :] == iota((SLOTS, steps), 0)
        token = jnp.sum(jnp.where(hit, local[t : t + 1, :] + 1, 0).astype(F32), axis=1, keepdims=True)
        chosen.append(ones_where(token.astype(I32) == iota((SLOTS, tokens), 1) + 1, BF16))
    for copy in copies:
        copy.wait()
    picked = jnp.zeros((SLOTS, hidden_ref.shape[2]), F32)
    for t in range(traces):
        picked += jnp.dot(chosen[t], hidden_ref[t], preferred_element_type=F32)
    depth = hidden_ref.shape[2] // (BLOCKS * NZH)
    pad = jnp.zeros((SLOTS, DEEP - depth), F32)
    for y0 in range(NY0):
        for low2 in range(NZ0 * NC):
            parts = []
            for zh in range(NZH):
                start = (y0 * 16 + zh * 4 + low2) * depth
                parts += [picked[:, start : start + depth], pad]
            piece = jnp.concatenate(parts, axis=1).astype(BF16)
            for yh in range(NYH):
                out_ref[yh * BLOCKS + y0 * 4 + low2] = piece


def layer_kernel(round_ref, boundary_ref, valid_ref, picks_ref, extra_ref, weight_ref, out_ref):
    low, window = round_ref[0], round_ref[1]
    traces, steps = boundary_ref.shape
    owner = jnp.where(valid_ref[...] == 1, boundary_ref[...] >> 6, -1)
    count = jnp.zeros((128, steps), F32)
    for t in range(traces):
        count += ones_where(owner[t : t + 1, :] == iota((128, steps), 0))
    count = jnp.sum(count, axis=1, keepdims=True)
    device = iota((128, 1), 0)
    most = jnp.max(count, axis=0, keepdims=True)
    fits = most <= SLOTS
    for group in range(NZH):
        crowd = jnp.sum(jnp.where(group_of(device) == group, count, 0.0), axis=0, keepdims=True)
        fits = fits & (crowd <= CAP)
    top = jnp.where(window > 0, window.astype(F32), jnp.where(fits, float(SLOTS), float(ROUND_SLOTS)))
    count = jnp.clip(count - low.astype(F32), 0.0, top)
    zh = lax.axis_index(ZH)
    mine = group_of(device) == zh
    count = jnp.where(mine, count, 0.0)
    place_in_group = (device >> 4) * 4 + (device & 3)
    lane = iota((128, OWNERS * SLOTS), 1) >> 4
    number = jnp.sum(jnp.where(lane == place_in_group, count, 0.0), axis=0, keepdims=True).astype(I32)
    start = jnp.sum(jnp.where(lane > place_in_group, count, 0.0), axis=0, keepdims=True).astype(I32)
    slot = iota((1, OWNERS * SLOTS), 1) & (SLOTS - 1)
    g = start + slot
    g = g + 2 * ((g >= PART).astype(I32) + (g >= 2 * PART).astype(I32) + (g >= 3 * PART).astype(I32))
    g = jnp.where(slot < number, g, -1)
    choose = ones_where(g == iota((NX * DEEP, OWNERS * SLOTS), 0), BF16)
    rows = jnp.dot(choose, picks_ref[...].reshape(OWNERS * SLOTS, 128), preferred_element_type=F32)
    pad = jnp.zeros((DEEP - weight_ref.shape[1], weight_ref.shape[2]), BF16)
    weight = []
    for source in range(NZH):
        weight += [weight_ref[(source & 1) * 2 + ((source >> 1) ^ (zh >> 1))], pad]
    partial = jnp.dot(rows.astype(BF16), jnp.concatenate(weight, axis=0), preferred_element_type=F32)
    for x in range(NX):
        for j in range(BLOCKS):
            columns = slice(j * 128, (j + 1) * 128)
            out_ref[x * BLOCKS + j] = partial[x * DEEP : (x + 1) * DEEP, columns]
            out_ref[x * BLOCKS + j, PART : PART + 1, :] = extra_ref[0, j : j + 1, :]
            out_ref[x * BLOCKS + j, PART + 1 : PART + 2, :] = extra_ref[1, j : j + 1, :]


def head_kernel(pre_ref, out_ref):
    pre = pre_ref[0]
    for source in range(1, NX * BLOCKS):
        pre = pre + pre_ref[source]
    extra = pre_ref[lax.axis_index("yh") * BLOCKS]
    unit = jnp.maximum(pre + extra[PART : PART + 1, :], 0.0) * extra[PART + 1 : PART + 2, :]
    unit = jnp.where(iota(unit.shape, 0) < PART, unit, 0.0)
    unit = jnp.concatenate([unit, jnp.zeros((128 - DEEP, 128), F32)], axis=0)
    logit = lax.dot_general(
        jnp.ones((8, 128), F32), unit, (((1,), (1,)), ((), ())), precision=HIGH, preferred_element_type=F32
    )
    out_ref[...] = jnp.broadcast_to(logit[0:1, :].reshape(1, 1, 128), out_ref.shape)


def spread_kernel(share_ref, out_ref):
    out_ref[...] = jnp.broadcast_to(jnp.sum(share_ref[...], axis=0, keepdims=True), out_ref.shape)


def finish_kernel(share_ref, place_ref, before_ref, valid_ref, pairs_ref, logit_ref, reward_ref, score_ref, margin_ref):
    each = share_ref.shape[0] // (NZH * NX)
    rows = []
    for group in range(NZH * NX):
        shares = share_ref[group * each : (group + 1) * each].reshape(each, 128)
        rows.append(jnp.sum(shares, axis=0, keepdims=True))
    place = place_ref[...]
    traces, steps = valid_ref.shape
    row, lane = place >> 7, place & 127
    found = jnp.zeros(place.shape, F32)
    for group in range(NZH * NX):
        here = jnp.take_along_axis(jnp.broadcast_to(rows[group], place.shape), lane, axis=1)
        found = jnp.where(row == group, here, found)
    logit = before_ref[...] + found[:, :steps]
    logit_ref[...] = logit
    live = valid_ref[...] == 1
    reward_ref[...] = jnp.where(live, logit, 0.0)
    score = jnp.min(jnp.where(live, logit, 1e30), axis=1, keepdims=True)
    diagonal = iota((traces, traces), 0) == iota((traces, traces), 1)
    flat = jnp.sum(jnp.where(diagonal, score, 0.0), axis=0, keepdims=True)
    score_ref[...] = flat
    trace = iota((traces, traces), 1)
    pairs = pairs_ref[...]
    ends = []
    for e in range(2):
        ends.append(jnp.sum(jnp.where(pairs[:, e : e + 1] == trace, flat, 0.0), axis=1, keepdims=True))
    margin_ref[...] = jnp.sum(jnp.where(diagonal, ends[0] - ends[1], 0.0), axis=0, keepdims=True)


def call(kernel, shapes, *args, scalars=0, far=0, scratch=()):
    single = not isinstance(shapes, list)
    near = len(args) - scalars - far
    return pl.pallas_call(
        kernel,
        out_shape=shapes,
        in_specs=[SMEM] * scalars + [VMEM] * near + [pl.BlockSpec(memory_space=pl.ANY)] * far,
        out_specs=VMEM if single else [VMEM] * len(shapes),
        scratch_shapes=scratch,
        compiler_params=pltpu.CompilerParams(vmem_limit_bytes=16 << 20),
    )(*args)


def array(shape, dtype=F32):
    return jax.ShapeDtypeStruct(shape, dtype)


def exchange(pieces, axes):
    return lax.all_to_all(pieces, axes, split_axis=0, concat_axis=0, tiled=True)


def per_device(hidden_states, boundary, valid, pairs, w_first, b_first, w_second):
    columns = w_first.shape[1]
    weights = []
    for flip in range(2):
        swap = []
        for a in range(NYH):
            for z in range(2):
                swap += [((a * 2 + z) * NX + b, (b * 2 + (z ^ flip)) * NX + a) for b in range(NX)]
        weights.append(lax.ppermute(w_first, ("yh", "z2", "x"), swap))
    weight = lax.all_gather(jnp.stack(weights), "z1").reshape(NZH, *w_first.shape)
    bias, second = b_first.reshape(8, columns // 8), w_second.reshape(8, columns // 8)

    def ranks(boundary, valid):
        owner = (boundary >> 6).reshape(-1)
        live = valid.reshape(-1) == 1
        order = jnp.arange(owner.shape[0], dtype=I32)
        same = (owner[:, None] == owner[None, :]) & live[None, :]
        rank = jnp.sum(same & (order[None, :] < order[:, None]), axis=1, dtype=I32)
        return owner, live, rank, group_of(owner)

    def limits(live, rank, group):
        most = jnp.max(jnp.where(live, rank + 1, 0))
        crowd = jnp.max(jnp.sum((group[:, None] == group[None, :]) & live[None, :], axis=1, dtype=I32))
        return most, jnp.where((most <= SLOTS) & (crowd <= CAP), SLOTS, ROUND_SLOTS).astype(I32)

    shape = array((OWNERS, SLOTS, 128), BF16)
    scratch = (pltpu.VMEM(hidden_states.shape, BF16), pltpu.SemaphoreType.DMA((3,)))

    def one_round(numbers, low, window, before, picks, extra):
        most = None
        picks = exchange(picks, ("yh", "y0", "z0", "c"))
        pre = call(
            layer_kernel, array((NX * BLOCKS, DEEP, 128)),
            numbers, boundary, valid, picks, extra, weight, scalars=1,
        )
        pre, late_boundary, late_valid = lax.optimization_barrier((pre, boundary, valid))
        owner, live, rank, group = ranks(late_boundary, late_valid)
        if window is None:
            most, window = limits(live, rank, group)
        pre = exchange(pre, ("x", "y0", "z0", "c"))
        share = exchange(call(head_kernel, array((NYH * NY0 * NC, 1, 128)), pre), ("yh", "y0", "c"))
        share = call(spread_kernel, array((NZH * NX * NZ0, 1, 128)), share)
        share = exchange(share, ZH + ("x", "z0"))
        inside = live & (rank >= low) & (rank < low + window)
        ahead = inside[None, :] & (group[None, :] == group[:, None]) & (owner[None, :] < owner[:, None])
        g = jnp.sum(ahead, axis=1, dtype=I32) + rank - low
        place = (group * NX + g // PART) * 128 + g % PART
        place = jnp.where(inside, place, -128).reshape(boundary.shape)
        place = jnp.pad(place, ((0, 0), (0, 128 - boundary.shape[1])), constant_values=-128)
        found = call(
            finish_kernel, [array(boundary.shape), array(boundary.shape), array((1, 8)), array((1, 8))],
            share, place, before, valid, pairs,
        )
        return found, most, window

    first = jnp.array([0, 0], I32)
    picks, extra = call(
        first_pick_kernel, [shape, array((2, 8, 128))],
        first, boundary, valid, hidden_states, bias, second, scalars=1, far=3, scratch=scratch,
    )
    found, most, window = one_round(first, 0, None, jnp.zeros(boundary.shape, F32), picks, extra)

    def more(state):
        low, found = state
        numbers = jnp.stack([low, jnp.int32(ROUND_SLOTS)])
        picks = call(
            pick_kernel, shape, numbers, boundary, valid, hidden_states, scalars=1, far=1, scratch=scratch
        )
        found, _, _ = one_round(numbers, low, ROUND_SLOTS, found[0], picks, extra)
        return low + ROUND_SLOTS, found

    _, found = lax.while_loop(lambda state: state[0] < most, more, (window, found))
    return found[1], found[2].reshape(8), found[3].reshape(8)


def solution(mesh):
    torus = Mesh(mesh.devices.reshape(NYH, NY0, 2, 2, NZ0, NC, NX), NAMES)
    return jax.shard_map(
        per_device,
        mesh=torus,
        in_specs=(P(None, SEQ, "x"), P(), P(), P(), P(SEQ, "x"), P("x"), P("x")),
        out_specs=(P(), P(), P()),
        check_vma=False,
    )
```

```python
import jax
import jax.numpy as jnp
from jax import lax
from jax.experimental import pallas as pl
from jax.experimental.pallas import tpu as pltpu
from jax.sharding import Mesh
from jax.sharding import PartitionSpec as P

NYH, NY0, NZH, NZ0, NC, NX = 4, 2, 4, 2, 2, 4
NAMES = ("yh", "y0", "z2", "z1", "z0", "c", "x")
SEQ = NAMES[:6]
ZH = ("z2", "z1")
OWNERS = NYH * NY0 * NZ0 * NC
BLOCKS = NY0 * NZ0 * NC
SLOTS = 16
ROUND_SLOTS = 3
PART = 30
CAP = NX * PART
DEEP = 32
VMEM = pl.BlockSpec(memory_space=pltpu.VMEM)
SMEM = pl.BlockSpec(memory_space=pltpu.SMEM)
F32, BF16, I32 = jnp.float32, jnp.bfloat16, jnp.int32
HIGH = lax.Precision.HIGHEST


def iota(shape, dim):
    return lax.broadcasted_iota(I32, shape, dim)


def ones_where(test, dtype=F32):
    return jnp.where(test, 1.0, 0.0).astype(dtype)


def group_of(owner):
    return (owner >> 2) & 3


def first_pick_kernel(round_ref, *refs):
    ends, bias_ref, second_ref, out_ref, extra_ref, *scratch = refs[:3], *refs[3:]
    sems = scratch[-1]
    copies = [
        pltpu.make_async_copy(bias_ref, extra_ref.at[0], sems.at[3]),
        pltpu.make_async_copy(second_ref, extra_ref.at[1], sems.at[4]),
    ]
    pick_kernel(round_ref, *ends, out_ref, *scratch, others=copies)


def pick_kernel(
    round_ref, far_boundary, far_valid, far_hidden, out_ref, boundary_ref, valid_ref, hidden_ref, sems, others=()
):
    copies = [
        pltpu.make_async_copy(far_boundary, boundary_ref, sems.at[0]),
        pltpu.make_async_copy(far_valid, valid_ref, sems.at[1]),
        pltpu.make_async_copy(far_hidden, hidden_ref, sems.at[2]),
        *others,
    ]
    for copy in copies:
        copy.start()
    me, low = lax.axis_index(SEQ), round_ref[0]
    traces, steps = boundary_ref.shape
    tokens = hidden_ref.shape[1]
    for copy in copies[:2]:
        copy.wait()
    local = boundary_ref[...] - me * tokens
    mine = (local >= 0) & (local < tokens) & (valid_ref[...] == 1)
    owned = ones_where(mine, BF16)
    before = ones_where(iota((steps, steps), 0) < iota((steps, steps), 1), BF16)
    within = jnp.dot(owned, before, preferred_element_type=F32)
    totals = jnp.dot(owned, jnp.ones((steps, steps), BF16), preferred_element_type=F32)
    earlier = ones_where(iota((traces, traces), 1) < iota((traces, traces), 0), BF16)
    carried = jnp.dot(earlier, totals.astype(BF16), preferred_element_type=F32)
    slot = jnp.where(mine, (within + carried).astype(I32) - low, -1)
    chosen = []
    for t in range(traces):
        hit = slot[t : t + 1, :] == iota((SLOTS, steps), 0)
        token = jnp.sum(jnp.where(hit, local[t : t + 1, :] + 1, 0).astype(F32), axis=1, keepdims=True)
        chosen.append(ones_where(token.astype(I32) == iota((SLOTS, tokens), 1) + 1, BF16))
    for copy in copies[2:]:
        copy.wait()
    picked = jnp.zeros((SLOTS, hidden_ref.shape[2]), F32)
    for t in range(traces):
        picked += jnp.dot(chosen[t], hidden_ref[t], preferred_element_type=F32)
    depth = hidden_ref.shape[2] // (BLOCKS * NZH)
    pad = jnp.zeros((SLOTS, DEEP - depth), F32)
    for y0 in range(NY0):
        for low2 in range(NZ0 * NC):
            parts = []
            for zh in range(NZH):
                start = (y0 * 16 + zh * 4 + low2) * depth
                parts += [picked[:, start : start + depth], pad]
            piece = jnp.concatenate(parts, axis=1).astype(BF16)
            for yh in range(NYH):
                out_ref[yh * BLOCKS + y0 * 4 + low2] = piece


def layer_kernel(round_ref, boundary_ref, valid_ref, picks_ref, extra_ref, weight_ref, out_ref):
    low, window = round_ref[0], round_ref[1]
    traces, steps = boundary_ref.shape
    owner = jnp.where(valid_ref[...] == 1, boundary_ref[...] >> 6, -1)
    count = jnp.zeros((128, steps), F32)
    for t in range(traces):
        count += ones_where(owner[t : t + 1, :] == iota((128, steps), 0))
    count = jnp.sum(count, axis=1, keepdims=True)
    device = iota((128, 1), 0)
    most = jnp.max(count, axis=0, keepdims=True)
    fits = most <= SLOTS
    for group in range(NZH):
        crowd = jnp.sum(jnp.where(group_of(device) == group, count, 0.0), axis=0, keepdims=True)
        fits = fits & (crowd <= CAP)
    top = jnp.where(window > 0, window.astype(F32), jnp.where(fits, float(SLOTS), float(ROUND_SLOTS)))
    count = jnp.clip(count - low.astype(F32), 0.0, top)
    zh = lax.axis_index(ZH)
    mine = group_of(device) == zh
    count = jnp.where(mine, count, 0.0)
    place_in_group = (device >> 4) * 4 + (device & 3)
    lane = iota((128, OWNERS * SLOTS), 1) >> 4
    number = jnp.sum(jnp.where(lane == place_in_group, count, 0.0), axis=0, keepdims=True).astype(I32)
    start = jnp.sum(jnp.where(lane > place_in_group, count, 0.0), axis=0, keepdims=True).astype(I32)
    slot = iota((1, OWNERS * SLOTS), 1) & (SLOTS - 1)
    g = start + slot
    g = g + 2 * ((g >= PART).astype(I32) + (g >= 2 * PART).astype(I32) + (g >= 3 * PART).astype(I32))
    g = jnp.where(slot < number, g, -1)
    choose = ones_where(g == iota((NX * DEEP, OWNERS * SLOTS), 0), BF16)
    rows = jnp.dot(choose, picks_ref[...].reshape(OWNERS * SLOTS, 128), preferred_element_type=F32)
    pad = jnp.zeros((DEEP - weight_ref.shape[1], weight_ref.shape[2]), BF16)
    weight = []
    for source in range(NZH):
        weight += [weight_ref[source], pad]
    partial = jnp.dot(rows.astype(BF16), jnp.concatenate(weight, axis=0), preferred_element_type=F32)
    for x in range(NX):
        for j in range(BLOCKS):
            columns = slice(j * 128, (j + 1) * 128)
            out_ref[x * BLOCKS + j] = partial[x * DEEP : (x + 1) * DEEP, columns]
            out_ref[x * BLOCKS + j, PART : PART + 1, :] = extra_ref[0, j : j + 1, :]
            out_ref[x * BLOCKS + j, PART + 1 : PART + 2, :] = extra_ref[1, j : j + 1, :]


def head_kernel(pre_ref, out_ref):
    pre = pre_ref[0]
    for source in range(1, NX * BLOCKS):
        pre = pre + pre_ref[source]
    extra = pre_ref[lax.axis_index("yh") * BLOCKS]
    unit = jnp.maximum(pre + extra[PART : PART + 1, :], 0.0) * extra[PART + 1 : PART + 2, :]
    unit = jnp.where(iota(unit.shape, 0) < PART, unit, 0.0)
    unit = jnp.concatenate([unit, jnp.zeros((128 - DEEP, 128), F32)], axis=0)
    logit = lax.dot_general(
        jnp.ones((8, 128), F32), unit, (((1,), (1,)), ((), ())), precision=HIGH, preferred_element_type=F32
    )
    out_ref[...] = jnp.broadcast_to(logit[0:1, :].reshape(1, 1, 128), out_ref.shape)


def spread_kernel(share_ref, out_ref):
    out_ref[...] = jnp.broadcast_to(jnp.sum(share_ref[...], axis=0, keepdims=True), out_ref.shape)


def finish_kernel(share_ref, place_ref, before_ref, valid_ref, pairs_ref, logit_ref, reward_ref, score_ref, margin_ref):
    each = share_ref.shape[0] // (NZH * NX)
    rows = []
    for group in range(NZH * NX):
        shares = share_ref[group * each : (group + 1) * each].reshape(each, 128)
        rows.append(jnp.sum(shares, axis=0, keepdims=True))
    place = place_ref[...]
    traces, steps = valid_ref.shape
    row, lane = place >> 7, place & 127
    found = jnp.zeros(place.shape, F32)
    for group in range(NZH * NX):
        here = jnp.take_along_axis(jnp.broadcast_to(rows[group], place.shape), lane, axis=1)
        found = jnp.where(row == group, here, found)
    logit = before_ref[...] + found[:, :steps]
    logit_ref[...] = logit
    live = valid_ref[...] == 1
    reward_ref[...] = jnp.where(live, logit, 0.0)
    score = jnp.min(jnp.where(live, logit, 1e30), axis=1, keepdims=True)
    diagonal = iota((traces, traces), 0) == iota((traces, traces), 1)
    flat = jnp.sum(jnp.where(diagonal, score, 0.0), axis=0, keepdims=True)
    score_ref[...] = flat
    trace = iota((traces, traces), 0)
    pairs = pairs_ref[...]
    ends = []
    for e in range(2):
        ends.append(jnp.sum(jnp.where(pairs[e : e + 1, :] == trace, score, 0.0), axis=0, keepdims=True))
    margin_ref[...] = ends[0] - ends[1]


def call(kernel, shapes, *args, scalars=0, far=0, scratch=()):
    single = not isinstance(shapes, list)
    near = len(args) - scalars - far
    return pl.pallas_call(
        kernel,
        out_shape=shapes,
        in_specs=[SMEM] * scalars + [VMEM] * near + [pl.BlockSpec(memory_space=pltpu.HBM)] * far,
        out_specs=VMEM if single else [VMEM] * len(shapes),
        scratch_shapes=scratch,
        compiler_params=pltpu.CompilerParams(vmem_limit_bytes=16 << 20),
    )(*args)


def array(shape, dtype=F32):
    return jax.ShapeDtypeStruct(shape, dtype)


def exchange(pieces, axes):
    return lax.all_to_all(pieces, axes, split_axis=0, concat_axis=0, tiled=True)


def per_device(hidden_states, boundary, valid, pairs, w_first, b_first, w_second):
    columns = w_first.shape[1]
    swap = [(a * NX + b, b * NX + a) for a in range(NYH) for b in range(NX)]
    weight = lax.ppermute(w_first, ("yh", "x"), swap)
    weight = lax.all_gather(weight, ZH)
    bias, second = b_first.reshape(8, columns // 8), w_second.reshape(8, columns // 8)

    def ranks(boundary, valid):
        owner = (boundary >> 6).reshape(-1)
        live = valid.reshape(-1) == 1
        order = jnp.arange(owner.shape[0], dtype=I32)
        same = (owner[:, None] == owner[None, :]) & live[None, :]
        rank = jnp.sum(same & (order[None, :] < order[:, None]), axis=1, dtype=I32)
        return owner, live, rank, group_of(owner)

    def limits(live, rank, group):
        most = jnp.max(jnp.where(live, rank + 1, 0))
        crowd = jnp.max(jnp.sum((group[:, None] == group[None, :]) & live[None, :], axis=1, dtype=I32))
        return most, jnp.where((most <= SLOTS) & (crowd <= CAP), SLOTS, ROUND_SLOTS).astype(I32)

    shape = array((OWNERS, SLOTS, 128), BF16)
    scratch = (
        pltpu.VMEM(boundary.shape, I32), pltpu.VMEM(valid.shape, I32), pltpu.VMEM(hidden_states.shape, BF16),
        pltpu.SemaphoreType.DMA((5,)),
    )

    def one_round(numbers, low, window, before, picks, extra):
        most = None
        picks = exchange(picks, ("yh", "y0", "z0", "c"))
        pre = call(
            layer_kernel, array((NX * BLOCKS, DEEP, 128)),
            numbers, boundary, valid, picks, extra, weight, scalars=1,
        )
        pre, late_boundary, late_valid, late_pairs = lax.optimization_barrier((pre, boundary, valid, pairs))
        pre = exchange(pre, ("x", "y0", "z0", "c"))
        owner, live, rank, group = ranks(late_boundary, late_valid)
        if window is None:
            most, window = limits(live, rank, group)
        inside = live & (rank >= low) & (rank < low + window)
        ahead = inside[None, :] & (group[None, :] == group[:, None]) & (owner[None, :] < owner[:, None])
        g = jnp.sum(ahead, axis=1, dtype=I32) + rank - low
        place = (group * NX + g // PART) * 128 + g % PART
        place = jnp.where(inside, place, -128).reshape(boundary.shape)
        place = jnp.pad(place, ((0, 0), (0, 128 - boundary.shape[1])), constant_values=-128)
        chosen = before, late_valid, jnp.pad(late_pairs.T, ((0, 6), (0, 0)))
        pre, place, chosen = lax.optimization_barrier((pre, place, chosen))
        share = exchange(call(head_kernel, array((NYH * NY0 * NC, 1, 128)), pre), ("yh", "y0", "c"))
        share = call(spread_kernel, array((NZH * NX * NZ0, 1, 128)), share)
        share = exchange(share, ZH + ("x", "z0"))
        found = call(
            finish_kernel, [array(boundary.shape), array(boundary.shape), array((1, 8)), array((1, 8))],
            share, place, *chosen,
        )
        return found, most, window

    first = jnp.array([0, 0], I32)
    picks, extra = call(
        first_pick_kernel, [shape, array((2, 8, 128))],
        first, boundary, valid, hidden_states, bias, second, scalars=1, far=5, scratch=scratch,
    )
    found, most, window = one_round(first, 0, None, jnp.zeros(boundary.shape, F32), picks, extra)

    def more(state):
        low, found = state
        numbers = jnp.stack([low, jnp.int32(ROUND_SLOTS)])
        picks = call(
            pick_kernel, shape, numbers, boundary, valid, hidden_states, scalars=1, far=3, scratch=scratch
        )
        found, _, _ = one_round(numbers, low, ROUND_SLOTS, found[0], picks, extra)
        return low + ROUND_SLOTS, found

    _, found = lax.while_loop(lambda state: state[0] < most, more, (window, found))
    return found[1], found[2].reshape(8), found[3].reshape(8)


def solution(mesh):
    torus = Mesh(mesh.devices.reshape(NYH, NY0, 2, 2, NZ0, NC, NX), NAMES)
    return jax.shard_map(
        per_device,
        mesh=torus,
        in_specs=(P(None, SEQ, "x"), P(), P(), P(), P(SEQ, "x"), P("x"), P("x")),
        out_specs=(P(), P(), P()),
        check_vma=False,
    )
```

```python
import jax
import jax.numpy as jnp
from jax import lax
from jax.experimental import pallas as pl
from jax.experimental.pallas import tpu as pltpu
from jax.sharding import Mesh
from jax.sharding import PartitionSpec as P

NYH, NY0, NZH, NZ0, NC, NX = 4, 2, 4, 2, 2, 4
NAMES = ("yh", "y0", "z2", "z1", "z0", "c", "x")
SEQ = NAMES[:6]
ZH = ("z2", "z1")
OWNERS = NYH * NY0 * NZ0 * NC
BLOCKS = NY0 * NZ0 * NC
SLOTS = 16
ROUND_SLOTS = 3
PART = 30
CAP = NX * PART
DEEP = 32
VMEM = pl.BlockSpec(memory_space=pltpu.VMEM)
SMEM = pl.BlockSpec(memory_space=pltpu.SMEM)
F32, BF16, I32 = jnp.float32, jnp.bfloat16, jnp.int32
HIGH = lax.Precision.HIGHEST


def iota(shape, dim):
    return lax.broadcasted_iota(I32, shape, dim)


def ones_where(test, dtype=F32):
    return jnp.where(test, 1.0, 0.0).astype(dtype)


def group_of(owner):
    return (owner >> 2) & 3


def first_pick_kernel(round_ref, *refs):
    inputs, bias_ref, second_ref, pairs_ref, out_ref, extra_ref, ends_ref, *scratch = refs[:3], *refs[3:]
    sems = scratch[-1]
    copies = [
        pltpu.make_async_copy(bias_ref, extra_ref.at[0], sems.at[3]),
        pltpu.make_async_copy(second_ref, extra_ref.at[1], sems.at[4]),
        pltpu.make_async_copy(pairs_ref, ends_ref, sems.at[5]),
    ]
    pick_kernel(round_ref, *inputs, out_ref, *scratch, others=copies)


def pick_kernel(
    round_ref, far_boundary, far_valid, far_hidden, out_ref, boundary_ref, valid_ref, hidden_ref, sems, others=()
):
    copies = [
        pltpu.make_async_copy(far_boundary, boundary_ref, sems.at[0]),
        pltpu.make_async_copy(far_valid, valid_ref, sems.at[1]),
        pltpu.make_async_copy(far_hidden, hidden_ref, sems.at[2]),
        *others,
    ]
    for copy in copies:
        copy.start()
    me, low = lax.axis_index(SEQ), round_ref[0]
    traces, steps = boundary_ref.shape
    tokens = hidden_ref.shape[1]
    for copy in copies[:2]:
        copy.wait()
    local = boundary_ref[...] - me * tokens
    mine = (local >= 0) & (local < tokens) & (valid_ref[...] == 1)
    owned = ones_where(mine, BF16)
    before = ones_where(iota((steps, steps), 0) < iota((steps, steps), 1), BF16)
    within = jnp.dot(owned, before, preferred_element_type=F32)
    totals = jnp.dot(owned, jnp.ones((steps, steps), BF16), preferred_element_type=F32)
    earlier = ones_where(iota((traces, traces), 1) < iota((traces, traces), 0), BF16)
    carried = jnp.dot(earlier, totals.astype(BF16), preferred_element_type=F32)
    slot = jnp.where(mine, (within + carried).astype(I32) - low, -1)
    chosen = []
    for t in range(traces):
        hit = slot[t : t + 1, :] == iota((SLOTS, steps), 0)
        token = jnp.sum(jnp.where(hit, local[t : t + 1, :] + 1, 0).astype(F32), axis=1, keepdims=True)
        chosen.append(ones_where(token.astype(I32) == iota((SLOTS, tokens), 1) + 1, BF16))
    for copy in copies[2:]:
        copy.wait()
    hidden = hidden_ref[...].reshape(traces * tokens, hidden_ref.shape[2])
    picked = jnp.dot(jnp.concatenate(chosen, axis=1), hidden, preferred_element_type=F32)
    depth = hidden_ref.shape[2] // (BLOCKS * NZH)
    pad = jnp.zeros((SLOTS, DEEP - depth), F32)
    for y0 in range(NY0):
        for low2 in range(NZ0 * NC):
            parts = []
            for zh in range(NZH):
                start = (y0 * 16 + zh * 4 + low2) * depth
                parts += [picked[:, start : start + depth], pad]
            piece = jnp.concatenate(parts, axis=1).astype(BF16)
            for yh in range(NYH):
                out_ref[yh * BLOCKS + y0 * 4 + low2] = piece


def layer_kernel(
    round_ref, boundary_ref, valid_ref, picks_ref, extra_ref, weight_ref, out_ref, place_ref, low_ref, most_ref
):
    low, window = round_ref[0], round_ref[1]
    traces, steps = boundary_ref.shape
    pad = jnp.full((traces, 128 - steps), -1, I32)
    owner = jnp.where(valid_ref[...] == 1, boundary_ref[...] >> 6, -1)
    lane = iota((traces, 128), 1)
    count = jnp.zeros((traces, 128), F32)
    for k in range(steps):
        count += ones_where(owner[:, k : k + 1] == lane)
    row, column = iota((128, 128), 0), iota((128, 128), 1)
    less = jnp.dot(count.astype(BF16), ones_where(row < column, BF16), preferred_element_type=F32)
    earlier = ones_where(iota((traces, traces), 1) < iota((traces, traces), 0), BF16)
    carried = jnp.dot(earlier, count.astype(BF16), preferred_element_type=F32)
    total = jnp.broadcast_to(jnp.sum(count, axis=0, keepdims=True), count.shape)
    most = jnp.max(total, axis=1, keepdims=True)
    fits = most <= SLOTS
    for group in range(NZH):
        crowd = jnp.sum(jnp.where(group_of(lane) == group, total, 0.0), axis=1, keepdims=True)
        fits = fits & (crowd <= CAP)
    top = jnp.where(window > 0, window.astype(F32), jnp.where(fits, float(SLOTS), float(ROUND_SLOTS)))
    most_ref[0] = most.astype(I32)[0, 0]
    low_ref[0] = low + top.astype(I32)[0, 0]
    taken = jnp.clip(total - low.astype(F32), 0.0, top)
    ahead = ones_where((row < column) & (group_of(row) == group_of(column)), BF16)
    start = jnp.dot(taken.astype(BF16), ahead, preferred_element_type=F32)

    where = jnp.concatenate([owner, pad], axis=1)
    index = jnp.maximum(where, 0)
    rank = jnp.take_along_axis(carried - less, index, axis=1) + lane.astype(F32) - low.astype(F32)
    g = (jnp.take_along_axis(start, index, axis=1) + rank).astype(I32)
    part = (g >= PART).astype(I32) + (g >= 2 * PART).astype(I32) + (g >= 3 * PART).astype(I32)
    place = (group_of(index) * NX + part) * 128 + g - PART * part
    place_ref[...] = jnp.where((where >= 0) & (rank >= 0.0) & (rank < top), place, -128)

    zh = lax.axis_index(ZH)
    slot = lane & (SLOTS - 1)
    choices = []
    for block in range(OWNERS * SLOTS // 128):
        device = (lane >> 4) + block * 8
        device = ((device >> 2) << 4) + (zh << 2) + (device & 3)
        g = jnp.take_along_axis(start, device, axis=1).astype(I32) + slot
        g = g + 2 * ((g >= PART).astype(I32) + (g >= 2 * PART).astype(I32) + (g >= 3 * PART).astype(I32))
        g = jnp.where(slot < jnp.take_along_axis(taken, device, axis=1).astype(I32), g, -1)
        choices.append(ones_where(g[0:1, :] == iota((NX * DEEP, 128), 0), BF16))
    choose = jnp.concatenate(choices, axis=1)
    rows = jnp.dot(choose, picks_ref[...].reshape(OWNERS * SLOTS, 128), preferred_element_type=F32)
    pad = jnp.zeros((DEEP - weight_ref.shape[1], weight_ref.shape[2]), BF16)
    weight = []
    for source in range(NZH):
        weight += [weight_ref[source], pad]
    partial = jnp.dot(rows.astype(BF16), jnp.concatenate(weight, axis=0), preferred_element_type=F32)
    for x in range(NX):
        for j in range(BLOCKS):
            columns = slice(j * 128, (j + 1) * 128)
            out_ref[x * BLOCKS + j] = partial[x * DEEP : (x + 1) * DEEP, columns]
            out_ref[x * BLOCKS + j, PART : PART + 1, :] = extra_ref[0, j : j + 1, :]
            out_ref[x * BLOCKS + j, PART + 1 : PART + 2, :] = extra_ref[1, j : j + 1, :]


def head_kernel(pre_ref, out_ref):
    pre = pre_ref[0]
    for source in range(1, NX * BLOCKS):
        pre = pre + pre_ref[source]
    extra = pre_ref[lax.axis_index("yh") * BLOCKS]
    unit = jnp.maximum(pre + extra[PART : PART + 1, :], 0.0) * extra[PART + 1 : PART + 2, :]
    unit = jnp.where(iota(unit.shape, 0) < PART, unit, 0.0)
    unit = jnp.concatenate([unit, jnp.zeros((128 - DEEP, 128), F32)], axis=0)
    logit = lax.dot_general(
        jnp.ones((8, 128), F32), unit, (((1,), (1,)), ((), ())), precision=HIGH, preferred_element_type=F32
    )
    out_ref[...] = jnp.broadcast_to(logit[0:1, :].reshape(1, 1, 128), out_ref.shape)


def spread_kernel(share_ref, out_ref):
    out_ref[...] = jnp.broadcast_to(jnp.sum(share_ref[...], axis=0, keepdims=True), out_ref.shape)


def finish_kernel(share_ref, place_ref, before_ref, valid_ref, pairs_ref, logit_ref, reward_ref, score_ref, margin_ref):
    each = share_ref.shape[0] // (NZH * NX)
    rows = []
    for group in range(NZH * NX):
        shares = share_ref[group * each : (group + 1) * each].reshape(each, 128)
        rows.append(jnp.sum(shares, axis=0, keepdims=True))
    place = place_ref[...]
    traces, steps = valid_ref.shape
    row, lane = place >> 7, place & 127
    found = jnp.zeros(place.shape, F32)
    for group in range(NZH * NX):
        here = jnp.take_along_axis(jnp.broadcast_to(rows[group], place.shape), lane, axis=1)
        found = jnp.where(row == group, here, found)
    logit = before_ref[...] + found[:, :steps]
    logit_ref[...] = logit
    live = valid_ref[...] == 1
    reward_ref[...] = jnp.where(live, logit, 0.0)
    score = jnp.min(jnp.where(live, logit, 1e30), axis=1, keepdims=True)
    diagonal = iota((traces, traces), 0) == iota((traces, traces), 1)
    flat = jnp.sum(jnp.where(diagonal, score, 0.0), axis=0, keepdims=True)
    score_ref[...] = flat
    trace = iota((traces, traces), 0)
    pairs = pairs_ref[...]
    ends = []
    for e in range(2):
        ends.append(jnp.sum(jnp.where(pairs[e : e + 1, :] == trace, score, 0.0), axis=0, keepdims=True))
    margin_ref[...] = ends[0] - ends[1]


def call(kernel, shapes, *args, scalars=0, far=0, scratch=(), scalars_out=0):
    single = not isinstance(shapes, list)
    near = len(args) - scalars - far
    return pl.pallas_call(
        kernel,
        out_shape=shapes,
        in_specs=[SMEM] * scalars + [VMEM] * near + [pl.BlockSpec(memory_space=pltpu.HBM)] * far,
        out_specs=VMEM if single else [VMEM] * (len(shapes) - scalars_out) + [SMEM] * scalars_out,
        scratch_shapes=scratch,
        compiler_params=pltpu.CompilerParams(vmem_limit_bytes=16 << 20),
    )(*args)


def array(shape, dtype=F32):
    return jax.ShapeDtypeStruct(shape, dtype)


def exchange(pieces, axes):
    return lax.all_to_all(pieces, axes, split_axis=0, concat_axis=0, tiled=True)


def per_device(hidden_states, boundary, valid, pairs, w_first, b_first, w_second):
    columns, traces = w_first.shape[1], boundary.shape[0]
    swap = [(a * NX + b, b * NX + a) for a in range(NYH) for b in range(NX)]
    weight = lax.ppermute(w_first, ("yh", "x"), swap)
    weight = lax.all_gather(weight, ZH)
    bias, second = b_first.reshape(8, columns // 8), w_second.reshape(8, columns // 8)

    shape = array((OWNERS, SLOTS, 128), BF16)
    scratch = (
        pltpu.VMEM(boundary.shape, I32), pltpu.VMEM(valid.shape, I32), pltpu.VMEM(hidden_states.shape, BF16),
        pltpu.SemaphoreType.DMA((6,)),
    )

    def one_round(numbers, before, picks, extra, ends):
        picks = exchange(picks, ("yh", "y0", "z0", "c"))
        pre, place, low, most = call(
            layer_kernel,
            [array((NX * BLOCKS, DEEP, 128)), array((traces, 128), I32)] + [array((1,), I32)] * 2,
            numbers, boundary, valid, picks, extra, weight, scalars=1, scalars_out=2,
        )
        pre = exchange(pre, ("x", "y0", "z0", "c"))
        share = exchange(call(head_kernel, array((NYH * NY0 * NC, 1, 128)), pre), ("yh", "y0", "c"))
        share = call(spread_kernel, array((NZH * NX * NZ0, 1, 128)), share)
        share = exchange(share, ZH + ("x", "z0"))
        found = call(
            finish_kernel, [array(boundary.shape), array(boundary.shape), array((1, 8)), array((1, 8))],
            share, place, before, valid, ends,
        )
        return found, low.reshape(()), most.reshape(())

    first = jnp.array([0, 0], I32)
    picks, extra, ends = call(
        first_pick_kernel, [shape, array((2, 8, 128)), array((2, traces), I32)],
        first, boundary, valid, hidden_states, bias, second, pairs.T, scalars=1, far=6, scratch=scratch,
    )
    found, low, most = one_round(first, jnp.zeros(boundary.shape, F32), picks, extra, ends)

    def more(state):
        low, found = state
        numbers = jnp.stack([low, jnp.int32(ROUND_SLOTS)])
        picks = call(
            pick_kernel, shape, numbers, boundary, valid, hidden_states, scalars=1, far=3, scratch=scratch
        )
        found, low, _ = one_round(numbers, found[0], picks, extra, ends)
        return low, found

    _, found = lax.while_loop(lambda state: state[0] < most, more, (low, found))
    return found[1], found[2].reshape(8), found[3].reshape(8)


def solution(mesh):
    torus = Mesh(mesh.devices.reshape(NYH, NY0, 2, 2, NZ0, NC, NX), NAMES)
    return jax.shard_map(
        per_device,
        mesh=torus,
        in_specs=(P(None, SEQ, "x"), P(), P(), P(), P(SEQ, "x"), P("x"), P("x")),
        out_specs=(P(), P(), P()),
        check_vma=False,
    )
```

```python
import jax
import jax.numpy as jnp
from jax import lax
from jax.experimental import pallas as pl
from jax.experimental.pallas import tpu as pltpu
from jax.sharding import Mesh
from jax.sharding import PartitionSpec as P

NYH, NY0, NZH, NZ0, NC, NX = 4, 2, 4, 2, 2, 4
NAMES = ("yh", "y0", "z2", "z1", "z0", "c", "x")
SEQ = NAMES[:6]
ZH = ("z2", "z1")
OWNERS = NYH * NY0 * NZ0 * NC
BLOCKS = NY0 * NZ0 * NC
SLOTS = 16
ROUND_SLOTS = 3
PART = 30
CAP = NX * PART
DEEP = 32
VMEM = pl.BlockSpec(memory_space=pltpu.VMEM)
SMEM = pl.BlockSpec(memory_space=pltpu.SMEM)
F32, BF16, I32 = jnp.float32, jnp.bfloat16, jnp.int32
HIGH = lax.Precision.HIGHEST


def iota(shape, dim):
    return lax.broadcasted_iota(I32, shape, dim)


def ones_where(test, dtype=F32):
    return jnp.where(test, 1.0, 0.0).astype(dtype)


def group_of(owner):
    return (owner >> 2) & 3


def first_pick_kernel(round_ref, *refs):
    ends, bias_ref, second_ref, out_ref, extra_ref, *scratch = refs[:3], *refs[3:]
    sems = scratch[-1]
    copies = [
        pltpu.make_async_copy(bias_ref, extra_ref.at[0], sems.at[3]),
        pltpu.make_async_copy(second_ref, extra_ref.at[1], sems.at[4]),
    ]
    pick_kernel(round_ref, *ends, out_ref, *scratch, others=copies)


def pick_kernel(
    round_ref, far_boundary, far_valid, far_hidden, out_ref, boundary_ref, valid_ref, hidden_ref, sems, others=()
):
    copies = [
        pltpu.make_async_copy(far_boundary, boundary_ref, sems.at[0]),
        pltpu.make_async_copy(far_valid, valid_ref, sems.at[1]),
        pltpu.make_async_copy(far_hidden, hidden_ref, sems.at[2]),
        *others,
    ]
    for copy in copies:
        copy.start()
    me, low = lax.axis_index(SEQ), round_ref[0]
    traces, steps = boundary_ref.shape
    tokens = hidden_ref.shape[1]
    for copy in copies[:2]:
        copy.wait()
    local = boundary_ref[...] - me * tokens
    mine = (local >= 0) & (local < tokens) & (valid_ref[...] == 1)
    owned = ones_where(mine, BF16)
    before = ones_where(iota((steps, steps), 0) < iota((steps, steps), 1), BF16)
    within = jnp.dot(owned, before, preferred_element_type=F32)
    totals = jnp.dot(owned, jnp.ones((steps, steps), BF16), preferred_element_type=F32)
    earlier = ones_where(iota((traces, traces), 1) < iota((traces, traces), 0), BF16)
    carried = jnp.dot(earlier, totals.astype(BF16), preferred_element_type=F32)
    slot = jnp.where(mine, (within + carried).astype(I32) - low, -1)
    chosen = []
    for t in range(traces):
        hit = slot[t : t + 1, :] == iota((SLOTS, steps), 0)
        token = jnp.sum(jnp.where(hit, local[t : t + 1, :] + 1, 0).astype(F32), axis=1, keepdims=True)
        chosen.append(ones_where(token.astype(I32) == iota((SLOTS, tokens), 1) + 1, BF16))
    for copy in copies[2:]:
        copy.wait()
    hidden = hidden_ref[...].reshape(traces * tokens, hidden_ref.shape[2])
    picked = jnp.dot(jnp.concatenate(chosen, axis=1), hidden, preferred_element_type=F32)
    depth = hidden_ref.shape[2] // (BLOCKS * NZH)
    pad = jnp.zeros((SLOTS, DEEP - depth), F32)
    for y0 in range(NY0):
        for low2 in range(NZ0 * NC):
            parts = []
            for zh in range(NZH):
                start = (y0 * 16 + zh * 4 + low2) * depth
                parts += [picked[:, start : start + depth], pad]
            piece = jnp.concatenate(parts, axis=1).astype(BF16)
            for yh in range(NYH):
                out_ref[yh * BLOCKS + y0 * 4 + low2] = piece


def layer_kernel(
    round_ref, boundary_ref, valid_ref, picks_ref, extra_ref, weight_ref, out_ref, place_ref, low_ref, most_ref
):
    low, window = round_ref[0], round_ref[1]
    traces, steps = boundary_ref.shape
    pad = jnp.full((traces, 128 - steps), -1, I32)
    owner = jnp.where(valid_ref[...] == 1, boundary_ref[...] >> 6, -1)
    lane = iota((traces, 128), 1)
    count = jnp.zeros((traces, 128), F32)
    for k in range(steps):
        count += ones_where(owner[:, k : k + 1] == lane)
    row, column = iota((128, 128), 0), iota((128, 128), 1)
    less = jnp.dot(count.astype(BF16), ones_where(row < column, BF16), preferred_element_type=F32)
    earlier = ones_where(iota((traces, traces), 1) < iota((traces, traces), 0), BF16)
    carried = jnp.dot(earlier, count.astype(BF16), preferred_element_type=F32)
    total = jnp.broadcast_to(jnp.sum(count, axis=0, keepdims=True), count.shape)
    most = jnp.max(total, axis=1, keepdims=True)
    fits = most <= SLOTS
    for group in range(NZH):
        crowd = jnp.sum(jnp.where(group_of(lane) == group, total, 0.0), axis=1, keepdims=True)
        fits = fits & (crowd <= CAP)
    top = jnp.where(window > 0, window.astype(F32), jnp.where(fits, float(SLOTS), float(ROUND_SLOTS)))
    most_ref[0] = most.astype(I32)[0, 0]
    low_ref[0] = low + top.astype(I32)[0, 0]
    taken = jnp.clip(total - low.astype(F32), 0.0, top)
    ahead = ones_where((row < column) & (group_of(row) == group_of(column)), BF16)
    start = jnp.dot(taken.astype(BF16), ahead, preferred_element_type=F32)

    where = jnp.concatenate([owner, pad], axis=1)
    index = jnp.maximum(where, 0)
    rank = jnp.take_along_axis(carried - less, index, axis=1) + lane.astype(F32) - low.astype(F32)
    g = (jnp.take_along_axis(start, index, axis=1) + rank).astype(I32)
    part = (g >= PART).astype(I32) + (g >= 2 * PART).astype(I32) + (g >= 3 * PART).astype(I32)
    place = (group_of(index) * NX + part) * 128 + g - PART * part
    place_ref[...] = jnp.where((where >= 0) & (rank >= 0.0) & (rank < top), place, -128)

    zh = lax.axis_index(ZH)
    slot = lane & (SLOTS - 1)
    choices = []
    for block in range(OWNERS * SLOTS // 128):
        device = (lane >> 4) + block * 8
        device = ((device >> 2) << 4) + (zh << 2) + (device & 3)
        g = jnp.take_along_axis(start, device, axis=1).astype(I32) + slot
        g = g + 2 * ((g >= PART).astype(I32) + (g >= 2 * PART).astype(I32) + (g >= 3 * PART).astype(I32))
        g = jnp.where(slot < jnp.take_along_axis(taken, device, axis=1).astype(I32), g, -1)
        choices.append(ones_where(g[0:1, :] == iota((NX * DEEP, 128), 0), BF16))
    choose = jnp.concatenate(choices, axis=1)
    rows = jnp.dot(choose, picks_ref[...].reshape(OWNERS * SLOTS, 128), preferred_element_type=F32)
    pad = jnp.zeros((DEEP - weight_ref.shape[1], weight_ref.shape[2]), BF16)
    weight = []
    for source in range(NZH):
        weight += [weight_ref[source], pad]
    partial = jnp.dot(rows.astype(BF16), jnp.concatenate(weight, axis=0), preferred_element_type=F32)
    for x in range(NX):
        for j in range(BLOCKS):
            columns = slice(j * 128, (j + 1) * 128)
            out_ref[x * BLOCKS + j] = partial[x * DEEP : (x + 1) * DEEP, columns]
            out_ref[x * BLOCKS + j, PART : PART + 1, :] = extra_ref[0, j : j + 1, :]
            out_ref[x * BLOCKS + j, PART + 1 : PART + 2, :] = extra_ref[1, j : j + 1, :]


def head_kernel(pre_ref, out_ref):
    pre = pre_ref[0]
    for source in range(1, NX * BLOCKS):
        pre = pre + pre_ref[source]
    extra = pre_ref[lax.axis_index("yh") * BLOCKS]
    unit = jnp.maximum(pre + extra[PART : PART + 1, :], 0.0) * extra[PART + 1 : PART + 2, :]
    unit = jnp.where(iota(unit.shape, 0) < PART, unit, 0.0)
    unit = jnp.concatenate([unit, jnp.zeros((128 - DEEP, 128), F32)], axis=0)
    logit = lax.dot_general(
        jnp.ones((8, 128), F32), unit, (((1,), (1,)), ((), ())), precision=HIGH, preferred_element_type=F32
    )
    out_ref[...] = jnp.broadcast_to(logit[0:1, :].reshape(1, 1, 128), out_ref.shape)


def spread_kernel(share_ref, out_ref):
    out_ref[...] = jnp.broadcast_to(jnp.sum(share_ref[...], axis=0, keepdims=True), out_ref.shape)


def finish_kernel(share_ref, place_ref, before_ref, valid_ref, pairs_ref, logit_ref, reward_ref, score_ref, margin_ref):
    each = share_ref.shape[0] // (NZH * NX)
    rows = []
    for group in range(NZH * NX):
        shares = share_ref[group * each : (group + 1) * each].reshape(each, 128)
        rows.append(jnp.sum(shares, axis=0, keepdims=True))
    place = place_ref[...]
    traces, steps = valid_ref.shape
    row, lane = place >> 7, place & 127
    found = jnp.zeros(place.shape, F32)
    for group in range(NZH * NX):
        here = jnp.take_along_axis(jnp.broadcast_to(rows[group], place.shape), lane, axis=1)
        found = jnp.where(row == group, here, found)
    logit = before_ref[...] + found[:, :steps]
    logit_ref[...] = logit
    live = valid_ref[...] == 1
    reward_ref[...] = jnp.where(live, logit, 0.0)
    score = jnp.min(jnp.where(live, logit, 1e30), axis=1, keepdims=True)
    diagonal = iota((traces, traces), 0) == iota((traces, traces), 1)
    flat = jnp.sum(jnp.where(diagonal, score, 0.0), axis=0, keepdims=True)
    score_ref[...] = flat
    trace = iota((traces, traces), 0)
    pairs = pairs_ref[...]
    ends = []
    for e in range(2):
        ends.append(jnp.sum(jnp.where(pairs[e : e + 1, :] == trace, score, 0.0), axis=0, keepdims=True))
    margin_ref[...] = ends[0] - ends[1]


def call(kernel, shapes, *args, scalars=0, far=0, scratch=(), scalars_out=0):
    single = not isinstance(shapes, list)
    near = len(args) - scalars - far
    return pl.pallas_call(
        kernel,
        out_shape=shapes,
        in_specs=[SMEM] * scalars + [VMEM] * near + [pl.BlockSpec(memory_space=pltpu.HBM)] * far,
        out_specs=VMEM if single else [VMEM] * (len(shapes) - scalars_out) + [SMEM] * scalars_out,
        scratch_shapes=scratch,
        compiler_params=pltpu.CompilerParams(vmem_limit_bytes=16 << 20),
    )(*args)


def array(shape, dtype=F32):
    return jax.ShapeDtypeStruct(shape, dtype)


def exchange(pieces, axes):
    return lax.all_to_all(pieces, axes, split_axis=0, concat_axis=0, tiled=True)


def per_device(hidden_states, boundary, valid, pairs, w_first, b_first, w_second):
    columns, traces = w_first.shape[1], boundary.shape[0]
    swap = [(a * NX + b, b * NX + a) for a in range(NYH) for b in range(NX)]
    weight = lax.ppermute(w_first, ("yh", "x"), swap)
    weight = lax.all_gather(weight, ZH)
    bias, second = b_first.reshape(8, columns // 8), w_second.reshape(8, columns // 8)

    shape = array((OWNERS, SLOTS, 128), BF16)
    scratch = (
        pltpu.VMEM(boundary.shape, I32), pltpu.VMEM(valid.shape, I32), pltpu.VMEM(hidden_states.shape, BF16),
        pltpu.SemaphoreType.DMA((5,)),
    )

    def one_round(numbers, before, picks, extra):
        picks = exchange(picks, ("yh", "y0", "z0", "c"))
        pre, place, low, most = call(
            layer_kernel,
            [array((NX * BLOCKS, DEEP, 128)), array((traces, 128), I32)] + [array((1,), I32)] * 2,
            numbers, boundary, valid, picks, extra, weight, scalars=1, scalars_out=2,
        )
        pre, late_pairs = lax.optimization_barrier((pre, pairs))
        pre = exchange(pre, ("x", "y0", "z0", "c"))
        low, most = jnp.maximum(low.reshape(()), 1), jnp.maximum(most.reshape(()), 0)
        ends = jnp.pad(late_pairs.T, ((0, 6), (0, 0)))
        pre, low, most, ends = lax.optimization_barrier((pre, low, most, ends))
        share = exchange(call(head_kernel, array((NYH * NY0 * NC, 1, 128)), pre), ("yh", "y0", "c"))
        share = call(spread_kernel, array((NZH * NX * NZ0, 1, 128)), share)
        share = exchange(share, ZH + ("x", "z0"))
        found = call(
            finish_kernel, [array(boundary.shape), array(boundary.shape), array((1, 8)), array((1, 8))],
            share, place, before, valid, ends,
        )
        return found, low, most

    first = jnp.array([0, 0], I32)
    picks, extra = call(
        first_pick_kernel, [shape, array((2, 8, 128))],
        first, boundary, valid, hidden_states, bias, second, scalars=1, far=5, scratch=scratch,
    )
    found, low, most = one_round(first, jnp.zeros(boundary.shape, F32), picks, extra)

    def more(state):
        low, found = state
        numbers = jnp.stack([low, jnp.int32(ROUND_SLOTS)])
        picks = call(
            pick_kernel, shape, numbers, boundary, valid, hidden_states, scalars=1, far=3, scratch=scratch
        )
        found, low, _ = one_round(numbers, found[0], picks, extra)
        return low, found

    _, found = lax.while_loop(lambda state: state[0] < most, more, (low, found))
    return found[1], found[2].reshape(8), found[3].reshape(8)


def solution(mesh):
    torus = Mesh(mesh.devices.reshape(NYH, NY0, 2, 2, NZ0, NC, NX), NAMES)
    return jax.shard_map(
        per_device,
        mesh=torus,
        in_specs=(P(None, SEQ, "x"), P(), P(), P(), P(SEQ, "x"), P("x"), P("x")),
        out_specs=(P(), P(), P()),
        check_vma=False,
    )
```
